32 devices in a mesh: dp: 4 (over y, core), tensor: 8 (over z, x).
Axes of the slice: x: 2, y: 2, z: 4, core: 2. Of those that a mesh axis runs over, the one named last changes fastest.
Arguments:
- ref_hidden: bfloat16 [1152, 4608], P('dp', 'tensor'), may hold values from -6 to 6
- pol_hidden: bfloat16 [1152, 4608], P('dp', 'tensor'), may hold values from -6 to 6
- readout: bfloat16 [1152, 4608], P('dp', 'tensor'), may hold values from -0.019897461 to 0.019897461
- lengths: int32 [12], P('dp'), may hold values from 16 to 96, as said below
- pairing: int32 [12], replicated, may hold values from 0 to 11, each once
- pre_gain: float32 [4608], replicated, may hold values from 0.25 to 1.75
- post_gain: float32 [4608], replicated, may hold values from 0.25 to 1.75
- w_query: bfloat16 [4608, 4096], P('dp', 'tensor'), may hold values from -0.09375 to 0.09375
- w_key: bfloat16 [4608, 2048], P('dp', 'tensor'), may hold values from -3 to 3
- value_projection: bfloat16 [4608, 2048], P('dp', 'tensor'), may hold values from -0.09375 to 0.09375
- w_out: bfloat16 [4608, 4096], P('dp', 'tensor'), may hold values from -0.09375 to 0.09375
- a_query: bfloat16 [4608, 64], P('dp'), may hold values from -0.09375 to 0.09375
- a_value: bfloat16 [4608, 64], P('dp'), may hold values from -0.09375 to 0.09375
- query_second_factor: bfloat16 [64, 4096], P(None, 'tensor'), may hold values from -0.75 to 0.75
- value_second_factor: bfloat16 [64, 2048], P(None, 'tensor'), may hold values from -0.75 to 0.75
Outputs:
- policy_out: bfloat16 [1152, 4608], P('dp', 'tensor')
- reference_out: bfloat16 [1152, 4608], P('dp', 'tensor')
- dpo_loss: float32 [], replicated
- grad_hidden: bfloat16 [1152, 4608], P('dp', 'tensor')
- grad_a: float32 [4608, 128], P('dp')
- query_factor_gradient: float32 [64, 4096], P(None, 'tensor')
- value_factor_gradient: float32 [64, 2048], P(None, 'tensor')
The draws below stay inside these ranges and needn't reach their ends.
Inputs may be any that keep to these rules, and one draw needn't show every extreme that they name: `lengths`: every sequence has at least one valid token and some sequence is full. `pairing`: entries 2k and 2k + 1 name the chosen and the rejected sequence of pair k; every sequence appears once.
All inputs are finite; a program needn't handle non-finite values.
Results may differ from the reference program's by a relative error of at most 0.0233.
The reference program's roundings to bfloat16 on the way count: a program that leaves them out, or rounds other values in their place, can miss the bound.
Values may be sent and summed in bfloat16 or wider, within the bound.
A program may use at most 128 MiB of HBM per device.

```python
import jax
import jax.numpy as jnp
from jax import lax

MODEL_WIDTH = 4608
HQ = 32
KEY_VALUE_HEADS = 16
HEAD_SIZE = 128
ADAPTER_RANK = 64
SEQUENCE_SLOTS = 96
SEQUENCE_COUNT = 12
TOKEN_SLOTS = 1152
N_TENSOR = 8


def draw_lengths(key, part):
    first_key = jax.random.fold_in(key, 11)
    second_key = jax.random.fold_in(key, 12)
    lowest = max(1, SEQUENCE_SLOTS // 6)
    drawn = jax.random.randint(first_key, (SEQUENCE_COUNT,), lowest, SEQUENCE_SLOTS + 1)
    target_row = jax.random.randint(second_key, (), 0, SEQUENCE_COUNT)
    return jnp.where(jnp.arange(SEQUENCE_COUNT) == target_row, SEQUENCE_SLOTS, drawn).astype(jnp.int32)


def key_head_scales(scale_random_key, lowest, highest):
    uniform_sample = jax.random.uniform(scale_random_key, (KEY_VALUE_HEADS,), jnp.float32)
    spread_heads = jnp.exp(jnp.log(lowest) + uniform_sample * (jnp.log(highest) - jnp.log(lowest)))
    return (spread_heads[:, None] * jnp.ones((1, HEAD_SIZE), jnp.float32)).reshape(KEY_VALUE_HEADS * HEAD_SIZE)


def draw_w_key(key, part):
    scale_random_key = jax.random.fold_in(key, 21)
    entry_random_key = jax.random.fold_in(key, 22)
    spread_heads = key_head_scales(scale_random_key, 1.0, 8.0)
    table_entries = jax.random.truncated_normal(entry_random_key, -3.0, 3.0, (MODEL_WIDTH, KEY_VALUE_HEADS * HEAD_SIZE), jnp.float32)
    return (table_entries * spread_heads[None, :] * float(MODEL_WIDTH) ** (-0.5)).astype(jnp.bfloat16)


def steps_of(own_key, dims, cuts, least, high):
    level = 1.0
    for dim, parts in cuts:
        steps = jax.random.uniform(jax.random.fold_in(jax.random.fold_in(own_key, 6), dim), (parts,), jnp.float32, least / len(cuts), high / len(cuts))
        level = level * jnp.repeat(jnp.exp(steps), dims[dim] // parts).reshape((-1,) + (1,) * (len(dims) - 1 - dim))
    return level


def gaussian(key, extent, deviation, limit, split=(), kind=jnp.bfloat16):
    entries = deviation * jax.random.normal(key, extent, jnp.float32)
    if split:
        entries = entries * steps_of(key, extent, split, -0.22, 0.18)
    return jnp.clip(entries, -limit, limit).astype(kind)


def setup_inputs(seed: int = 0) -> dict:
    splits = jax.random.split(jax.random.key(seed), 16)
    return {
        "ref_hidden": gaussian(splits[0], (TOKEN_SLOTS, MODEL_WIDTH), 1.0, 6.0, ((0, 4), (1, 8))),
        "pol_hidden": gaussian(splits[1], (TOKEN_SLOTS, MODEL_WIDTH), 1.0, 6.0, ((0, 4), (1, 8))),
        "readout": gaussian(splits[2], (TOKEN_SLOTS, MODEL_WIDTH), 0.003, 0.019897461, ((0, 4), (1, 8))),
        "lengths": draw_lengths(jax.random.fold_in(splits[15], 71), 0),
        "pairing": jax.random.permutation(splits[4], SEQUENCE_COUNT).astype(jnp.int32),
        "pre_gain": jnp.clip(1.0 + 0.15 * jax.random.normal(splits[5], (MODEL_WIDTH,), jnp.float32), 0.25, 1.75),
        "post_gain": jnp.clip(1.0 + 0.15 * jax.random.normal(splits[6], (MODEL_WIDTH,), jnp.float32), 0.25, 1.75),
        "w_query": gaussian(splits[7], (MODEL_WIDTH, HQ * HEAD_SIZE), MODEL_WIDTH ** -0.5, 0.09375, ((0, 4), (1, 8))),
        "w_key": draw_w_key(jax.random.fold_in(splits[15], 71), 0),
        "value_projection": gaussian(splits[9], (MODEL_WIDTH, KEY_VALUE_HEADS * HEAD_SIZE), MODEL_WIDTH ** -0.5, 0.09375, ((0, 4), (1, 8))),
        "w_out": gaussian(splits[10], (MODEL_WIDTH, HQ * HEAD_SIZE), (HQ * HEAD_SIZE) ** -0.5, 0.09375, ((0, 4), (1, 8))),
        "a_query": gaussian(splits[11], (MODEL_WIDTH, ADAPTER_RANK), MODEL_WIDTH ** -0.5, 0.09375, ((0, 4),)),
        "a_value": gaussian(splits[12], (MODEL_WIDTH, ADAPTER_RANK), MODEL_WIDTH ** -0.5, 0.09375, ((0, 4),)),
        "query_second_factor": gaussian(splits[13], (ADAPTER_RANK, HQ * HEAD_SIZE), ADAPTER_RANK ** -0.5, 0.75, ((1, 8),)),
        "value_second_factor": gaussian(splits[14], (ADAPTER_RANK, KEY_VALUE_HEADS * HEAD_SIZE), ADAPTER_RANK ** -0.5, 0.75, ((1, 8),)),
    }


NORM_EPS = 1e-06
SOFT_CAP = 50.0
ADAPTER_SCALE = 0.5
DPO_BETA = 0.5
LOSS_SCALE = 256.0
ROPE_BASE = 10000.0

def query_scale():
    return float(MODEL_WIDTH // HQ) ** (-0.5)

def apply_rotation(value_rows, direction):
    length = value_rows.shape[1]
    head_depth = value_rows.shape[3]
    middle = head_depth // 2
    spacing = ROPE_BASE ** (-2.0 * jnp.arange(middle, dtype=jnp.float32) / head_depth)
    angles = jnp.arange(length, dtype=jnp.float32)[:, None] * spacing[None, :]
    cosine = jnp.cos(angles)[None, :, None, :]
    sine_part = direction * jnp.sin(angles)[None, :, None, :]
    leading = value_rows[..., :middle]
    trailing = value_rows[..., middle:]
    return jnp.concatenate([leading * cosine - trailing * sine_part, trailing * cosine + leading * sine_part], axis=-1)

def allowed_mask(lengths, length):
    places = jnp.arange(length)
    causal = places[None, :] <= places[:, None]
    living = places[None, :] < lengths[:, None]
    return causal[None, None, None, :, :] & living[:, None, None, None, :]

def attend(query_rows, rotated_keys, value_rows, lengths):
    seqs_here, length, q_heads, head_depth = query_rows.shape
    kv_heads = rotated_keys.shape[2]
    grouped_heads = query_rows.reshape(seqs_here, length, kv_heads, q_heads // kv_heads, head_depth)
    scores = jnp.einsum('sqkgd,spkd->skgqp', grouped_heads.astype(jnp.float32), rotated_keys.astype(jnp.float32)) * query_scale()
    capped = SOFT_CAP * jnp.tanh(scores / SOFT_CAP)
    allowed = allowed_mask(lengths, length)
    weights = jnp.where(allowed, jnp.exp(capped), 0.0)
    probabilities = weights / lax.optimization_barrier(jnp.sum(weights, axis=-1, keepdims=True))
    probs_low = probabilities.astype(jnp.bfloat16)
    mixed_out = jnp.einsum('skgqp,spkd->sqkgd', probs_low.astype(jnp.float32), value_rows.astype(jnp.float32))
    return (mixed_out.astype(jnp.bfloat16).reshape(seqs_here, length, q_heads, head_depth), probs_low, probabilities, capped)

def attend_back(grad_mixed, query_rows, rotated_keys, value_rows, probs_low, probabilities, capped):
    seqs_here, length, q_heads, head_depth = query_rows.shape
    kv_heads = rotated_keys.shape[2]
    shape_five = (seqs_here, length, kv_heads, q_heads // kv_heads, head_depth)
    grouped_heads = query_rows.reshape(shape_five).astype(jnp.float32)
    grad_grouped = grad_mixed.reshape(shape_five).astype(jnp.float32)
    grad_probs = jnp.einsum('sqkgd,spkd->skgqp', grad_grouped, value_rows.astype(jnp.float32))
    value_rows_gradient = jnp.einsum('skgqp,sqkgd->spkd', probs_low.astype(jnp.float32), grad_grouped)
    centered = grad_probs - lax.optimization_barrier(jnp.sum(grad_probs * probabilities, axis=-1, keepdims=True))
    grad_scores = (probabilities * centered * (1.0 - (capped / SOFT_CAP) ** 2) * query_scale()).astype(jnp.bfloat16)
    grad_scores = grad_scores.astype(jnp.float32)
    query_rows_gradient = jnp.einsum('skgqp,spkd->sqkgd', grad_scores, rotated_keys.astype(jnp.float32)).reshape(seqs_here, length, q_heads, head_depth)
    key_rows_gradient = jnp.einsum('skgqp,sqkgd->spkd', grad_scores, grouped_heads)
    return (query_rows_gradient, key_rows_gradient, value_rows_gradient)

def normalize(hidden, gain):
    wide_rows = hidden.astype(jnp.float32)
    pre_scale = lax.rsqrt(lax.optimization_barrier(jnp.sum(wide_rows * wide_rows, axis=1, keepdims=True)) / MODEL_WIDTH + NORM_EPS)
    return ((wide_rows * pre_scale * gain).astype(jnp.bfloat16), pre_scale)

def attention_layer(hidden, normed, lengths, post_gain, w_query, w_key, value_projection, w_out, adapters):
    query_rows = jnp.dot(normed, w_query, preferred_element_type=jnp.float32)
    keys_before_rotation = jnp.dot(normed, w_key, preferred_element_type=jnp.float32)
    value_rows = jnp.dot(normed, value_projection, preferred_element_type=jnp.float32)
    low_rank_update = None
    if adapters is not None:
        a_query, a_value, query_second_factor, value_second_factor = adapters
        low_rank_update = jnp.dot(normed, jnp.concatenate([a_query, a_value], axis=1), preferred_element_type=jnp.float32).astype(jnp.bfloat16)
        query_rows = query_rows + ADAPTER_SCALE * jnp.dot(low_rank_update[:, :ADAPTER_RANK], query_second_factor, preferred_element_type=jnp.float32)
        value_rows = value_rows + ADAPTER_SCALE * jnp.dot(low_rank_update[:, ADAPTER_RANK:], value_second_factor, preferred_element_type=jnp.float32)
    query_rows = apply_rotation(query_rows.reshape(SEQUENCE_COUNT, SEQUENCE_SLOTS, HQ, HEAD_SIZE), 1.0).astype(jnp.bfloat16)
    rotated_keys = apply_rotation(keys_before_rotation.reshape(SEQUENCE_COUNT, SEQUENCE_SLOTS, KEY_VALUE_HEADS, HEAD_SIZE), 1.0).astype(jnp.bfloat16)
    value_rows = value_rows.reshape(SEQUENCE_COUNT, SEQUENCE_SLOTS, KEY_VALUE_HEADS, HEAD_SIZE).astype(jnp.bfloat16)
    mixed_out, probs_low, probabilities, capped = attend(query_rows, rotated_keys, value_rows, lengths)
    flat_mixed = mixed_out.reshape(TOKEN_SLOTS, HQ * HEAD_SIZE)
    group_cols = HQ * HEAD_SIZE // N_TENSOR
    contract_cols = (((1,), (1,)), ((), ()))

    def add_group(index_g, running):
        start = (index_g * group_cols).astype(jnp.int32)
        columns = lax.dynamic_slice_in_dim(flat_mixed, start, group_cols, 1)
        w_columns = lax.dynamic_slice_in_dim(w_out, start, group_cols, 1)
        term_low = lax.dot_general(columns, w_columns, contract_cols, preferred_element_type=jnp.float32).astype(jnp.bfloat16)
        return running + lax.optimization_barrier(term_low).astype(jnp.float32)
    summed = lax.fori_loop(jnp.int32(0), jnp.int32(N_TENSOR), add_group, jnp.zeros((TOKEN_SLOTS, MODEL_WIDTH), jnp.float32))
    post_scale = lax.rsqrt(lax.optimization_barrier(jnp.sum(summed * summed, axis=1, keepdims=True)) / MODEL_WIDTH + NORM_EPS)
    result = hidden.astype(jnp.float32) + summed * post_scale * post_gain
    saved = (low_rank_update, query_rows, rotated_keys, value_rows, probs_low, probabilities, capped, summed, post_scale)
    return (result, saved)

def block_hook(grads, factor):
    grouped_heads = grads.astype(jnp.float32).reshape(TOKEN_SLOTS, N_TENSOR, -1)
    grouped_factors = factor.astype(jnp.float32).reshape(ADAPTER_RANK, N_TENSOR, -1)
    split_pieces = (ADAPTER_SCALE * jnp.einsum('fei,kei->fek', grouped_heads, grouped_factors)).astype(jnp.bfloat16)
    return lax.optimization_barrier(jnp.sum(lax.optimization_barrier(split_pieces).astype(jnp.float32), axis=1))

def reference(ref_hidden, pol_hidden, readout, lengths, pairing, pre_gain, post_gain, w_query, w_key, value_projection, w_out, a_query, a_value, query_second_factor, value_second_factor):
    ref_normed, ref_scale = normalize(ref_hidden, pre_gain)
    ref_result, ref_saved = attention_layer(ref_hidden, ref_normed, lengths, post_gain, w_query, w_key, value_projection, w_out, None)
    pol_normed, pol_scale = normalize(pol_hidden, pre_gain)
    pol_result, pol_saved = attention_layer(pol_hidden, pol_normed, lengths, post_gain, w_query, w_key, value_projection, w_out, (a_query, a_value, query_second_factor, value_second_factor))
    readout_wide = readout.astype(jnp.float32)
    living = (jnp.arange(SEQUENCE_SLOTS)[None, :] < lengths[:, None]).astype(jnp.float32)

    def sequence_score(result):
        return lax.optimization_barrier(jnp.sum(lax.optimization_barrier(jnp.sum(result * readout_wide, axis=1)).reshape(SEQUENCE_COUNT, SEQUENCE_SLOTS) * living, axis=1))
    ratios = sequence_score(pol_result) - sequence_score(ref_result)
    chosen = pairing[0::2]
    rejected = pairing[1::2]
    margins = DPO_BETA * (ratios[chosen] - ratios[rejected])
    dpo_loss = jnp.sum(jax.nn.softplus(-margins))
    pair_pull = DPO_BETA * LOSS_SCALE * jax.nn.sigmoid(-margins)
    coefficients = jnp.zeros((SEQUENCE_COUNT,), jnp.float32).at[chosen].add(-pair_pull).at[rejected].add(pair_pull)
    grad_result = (coefficients[:, None] * living).reshape(TOKEN_SLOTS, 1) * readout_wide
    low_rank_update, query_rows, rotated_keys, value_rows, probs_low, probabilities, capped, summed, post_scale = pol_saved
    post_dot = lax.optimization_barrier(jnp.sum(summed * post_gain * grad_result, axis=1, keepdims=True))
    grad_summed = post_scale * post_gain * grad_result - summed * post_scale ** 3 * post_dot / MODEL_WIDTH
    grad_wide = grad_summed.astype(jnp.bfloat16)
    grad_mixed = jnp.dot(grad_wide, w_out, preferred_element_type=jnp.float32).astype(jnp.bfloat16)
    grad_q_rot, rotated_key_gradient, value_head_gradient = attend_back(grad_mixed.reshape(SEQUENCE_COUNT, SEQUENCE_SLOTS, HQ, HEAD_SIZE), query_rows, rotated_keys, value_rows, probs_low, probabilities, capped)
    query_rows_gradient = apply_rotation(grad_q_rot, -1.0).reshape(TOKEN_SLOTS, HQ * HEAD_SIZE).astype(jnp.bfloat16)
    key_rows_gradient = apply_rotation(rotated_key_gradient, -1.0).reshape(TOKEN_SLOTS, KEY_VALUE_HEADS * HEAD_SIZE).astype(jnp.bfloat16)
    value_rows_gradient = value_head_gradient.reshape(TOKEN_SLOTS, KEY_VALUE_HEADS * HEAD_SIZE).astype(jnp.bfloat16)
    rows_contraction = (((0,), (0,)), ((), ()))
    contract_cols = (((1,), (1,)), ((), ()))
    query_factor_gradient = ADAPTER_SCALE * lax.dot_general(low_rank_update[:, :ADAPTER_RANK], query_rows_gradient, rows_contraction, preferred_element_type=jnp.float32)
    value_factor_gradient = ADAPTER_SCALE * lax.dot_general(low_rank_update[:, ADAPTER_RANK:], value_rows_gradient, rows_contraction, preferred_element_type=jnp.float32)
    adapter_grad = jnp.concatenate([block_hook(query_rows_gradient, query_second_factor), block_hook(value_rows_gradient, value_second_factor)], axis=1)
    grad_a = lax.dot_general(pol_normed.astype(jnp.float32), adapter_grad, rows_contraction, precision=lax.Precision.HIGHEST)
    a_both = jnp.concatenate([a_query, a_value], axis=1).astype(jnp.float32)
    grad_normed = lax.dot_general(query_rows_gradient, w_query, contract_cols, preferred_element_type=jnp.float32)
    grad_normed = grad_normed + lax.dot_general(key_rows_gradient, w_key, contract_cols, preferred_element_type=jnp.float32)
    grad_normed = grad_normed + lax.dot_general(value_rows_gradient, value_projection, contract_cols, preferred_element_type=jnp.float32)
    grad_normed = grad_normed + lax.dot_general(adapter_grad, a_both, contract_cols, precision=lax.Precision.HIGHEST)
    narrow = pol_hidden.astype(jnp.float32)
    pre_dot = lax.optimization_barrier(jnp.sum(narrow * pre_gain * grad_normed, axis=1, keepdims=True))
    grad_hidden = grad_result + pol_scale * pre_gain * grad_normed - narrow * pol_scale ** 3 * pre_dot / MODEL_WIDTH
    return (pol_result.astype(jnp.bfloat16), ref_result.astype(jnp.bfloat16), dpo_loss, grad_hidden.astype(jnp.bfloat16), grad_a, query_factor_gradient, value_factor_gradient)
```

```python
import jax
import jax.numpy as jnp
import numpy as np
from jax import lax
from jax.experimental import pallas as pl
from jax.experimental.pallas import tpu as pltpu
from jax.sharding import PartitionSpec as P

MODEL_WIDTH = 4608
HQ = 32
HEAD_SIZE = 128


NORM_EPS = 1e-06
SOFT_CAP = 50.0
ADAPTER_SCALE = 0.5
DPO_BETA = 0.5
LOSS_SCALE = 256.0
ROPE_BASE = 10000.0

MESH = pl.DeviceIdType.MESH
VMEM_GRANT = 67_000_000
LANES = 128
f32, bf16 = jnp.float32, jnp.bfloat16
NT = (((1,), (1,)), ((), ()))
TN = (((0,), (0,)), ((), ()))


def query_scale():
    return float(MODEL_WIDTH // HQ) ** (-0.5)


def grid_of(axis, count):
    if axis == "dp":
        inner = 2 if count % 2 == 0 else 1
    else:
        inner = 1
        while (inner * 2) ** 2 <= count and count % (inner * 2) == 0:
            inner *= 2
    return count // inner, inner


def pick(size, options):
    for option in options:
        if size % option == 0:
            return option
    return size


def rope_tables(length):
    half = HEAD_SIZE // 2
    spacing = ROPE_BASE ** (-2.0 * np.arange(half, dtype=np.float32) / HEAD_SIZE)
    angles = np.arange(length, dtype=np.float32)[:, None] * spacing[None, :].astype(np.float32)
    cosine, sine = np.cos(angles), np.sin(angles)
    return (
        np.concatenate([cosine, cosine], axis=1).astype(np.float32),
        np.concatenate([-sine, sine], axis=1).astype(np.float32),
    )


def dot(x, y, dims=(((1,), (0,)), ((), ()))):
    return lax.dot_general(x, y, dims, preferred_element_type=f32)


def remote(src, dst, send_sem, recv_sem, axis, rank):
    return pltpu.make_async_remote_copy(
        src_ref=src,
        dst_ref=dst,
        send_sem=send_sem,
        recv_sem=recv_sem,
        device_id={axis: rank},
        device_id_type=MESH,
    )


class Sizes:
    def __init__(self, tok_rows, part_width, seqs, dp, tensor, q_cols, k_cols, rank):
        self.R, self.PW, self.S, self.D, self.T = tok_rows, part_width, seqs, dp, tensor
        self.L = tok_rows // seqs
        self.QC, self.KC = q_cols, k_cols
        self.AR = 2 * rank
        self.rank = rank
        self.NC = q_cols + 2 * k_cols
        self.NW = self.NC + self.AR
        self.O, self.I = grid_of("tensor", tensor)
        self.Y, self.C = grid_of("dp", dp)
        self.r = tensor // dp
        self.gp = max(self.O // self.Y, 1)
        self.KV = k_cols // HEAD_SIZE
        self.G = q_cols // k_cols
        self.P = self.L
        self.n = tok_rows // self.P
        self.Rp = -(-tok_rows // LANES) * LANES
        self.W = part_width * tensor
        self.step = pick(tok_rows, (48, 32, 16))
        size = 16
        while tok_rows % size or tok_rows // size > tensor:
            size += 16
        self.HR, self.HN = size, tok_rows // size


def vm(*shape, kind=bf16):
    return pltpu.VMEM(shape, kind)


def sem(*counts):
    return [pltpu.SemaphoreType.DMA((max(count, 1),)) for count in counts]


def build_scratch(z):
    R, PW, T, D, O, I, n = z.R, z.PW, z.T, z.D, z.O, z.I, z.n
    inner = O * (I - 1)
    moved = z.QC + z.KC

    def boxes():
        return [vm(T, R, PW), vm(max(inner, 1), R, PW), vm(O, R, PW), vm(O, R, PW)]

    def reduce_sems():
        return sem(inner * n, inner * n, O * n, O * n, O * n)

    def gather_sems(count):
        return sem(T * count, O * count, O * count, inner * count)

    def stat():
        return [vm(T, 8, z.Rp, kind=f32), vm(8, z.Rp, kind=f32)] + sem(T, T)

    def weight_sems():
        return sem(D * z.r, (z.Y - 1) * z.r, z.Y * (z.C - 1) * z.r)

    return dict(
        held=vm(T, 2 * R, PW),
        normed=vm(T, 2 * R, PW),
        W=vm(D, z.r * PW, z.NW),
        WO=vm(D, z.r * PW, z.QC),
        acc=vm(2 * R, z.NW, kind=f32),
        added=vm(R, moved, kind=f32),
        low=vm(R, z.AR),
        F=vm(z.AR, moved),
        q2=vm(z.S, z.KV, z.G * z.L, HEAD_SIZE),
        kk=vm(z.S, z.KV, z.L, HEAD_SIZE),
        vv=vm(z.S, z.KV, z.L, HEAD_SIZE),
        probs=vm(z.S, z.KV, z.G * z.L, z.L, kind=f32),
        capped=vm(z.S, z.KV, z.G * z.L, z.L, kind=f32),
        mixed=vm(2 * R, z.QC),
        pol=boxes(),
        ref=boxes(),
        pol_sems=reduce_sems(),
        ref_sems=reduce_sems(),
        grad_sems=reduce_sems(),
        piece=vm(z.P, PW, kind=f32),
        summed=vm(2 * R, PW, kind=f32),
        gheld=vm(T, R, PW),
        gm=vm(R, z.QC, kind=f32),
        gmb=vm(R, z.QC),
        dcat=vm(R, z.NW),
        gnorm=vm(R, PW, kind=f32),
        col=vm(2 * R, 1, kind=f32),
        scol=vm(2 * R, 1, kind=f32),
        liv=vm(R, 1, kind=f32),
        ccol=vm(R, 1, kind=f32),
        pcol=vm(4 * R, 1, kind=f32),
        s0=stat(),
        s1=stat(),
        s2=stat(),
        s3=stat(),
        score=[vm(D, 8, LANES, kind=f32), vm(8, LANES, kind=f32)] + sem(D, D),
        hbox=vm(T, z.HR, z.AR),
        hsum=vm(z.HN, z.HR, z.AR),
        h1=sem(T, T),
        h2=sem(T, T),
        fac=[vm(D, z.rank, moved), vm(z.rank, moved)] + sem(D, D),
        ad=[vm(D, z.r * PW, z.AR), vm(D, z.r * PW, z.AR)] + sem(D, D),
        load=sem(8),
        hid=[gather_sems(n), gather_sems(n)],
        gag=gather_sems(n),
        wq=weight_sems(),
        wo=weight_sems(),
    )


class Refs:
    pass


class Gather:
    def __init__(self, z, place, held, sems, row=0):
        self.z, self.place, self.held, self.pieces = z, place, held, z.n
        self.r, self.u, self.d, self.x = sems
        self.row = row

    def block(self, slot, c):
        return self.held.at[slot, pl.ds(self.row + c * self.z.P, self.z.P)]

    def copy(self, aa, c, kind, k=0):
        z, (a, b) = self.z, self.place
        slot = aa * z.I + b
        block = self.block(slot, c)
        at = aa * self.pieces + c
        if kind == "up":
            send, rank = self.u.at[at], lax.rem(a + 1, z.O) * z.I + b
        elif kind == "dn":
            send, rank = self.d.at[at], lax.rem(a + z.O - 1, z.O) * z.I + b
        else:
            send = self.x.at[(aa * (z.I - 1) + k - 1) * self.pieces + c]
            rank = a * z.I + lax.rem(b + k, z.I)
        return remote(block, block, send, self.r.at[slot * self.pieces + c], "tensor", rank)

    def wait_recv(self, slot, c):
        z = self.z
        block = self.block(slot, c)
        at = slot * self.pieces + c
        remote(block, block, self.u.at[0], self.r.at[at], "tensor", 0).wait_recv()

    def sends(self, aa, c, act):
        z, (a, b) = self.z, self.place

        @pl.when((aa <= a) & (a < z.O - 1))
        def _():
            act(self.copy(aa, c, "up"))

        @pl.when((aa >= a) & (a > 0))
        def _():
            act(self.copy(aa, c, "dn"))

        for k in range(1, z.I):
            act(self.copy(aa, c, "x", k))

    def start(self):
        for c in range(self.pieces):
            self.sends(self.place[0], c, lambda copy: copy.start())

    def relay(self, aa):
        z, (a, b) = self.z, self.place

        @pl.loop(0, self.pieces)
        def _(c):
            self.wait_recv(aa * z.I + b, c)
            self.sends(aa, c, lambda copy: copy.start())

    def wait_inner(self, aa):
        z, (a, b) = self.z, self.place
        for k in range(1, z.I):

            @pl.loop(0, self.pieces)
            def _(c, k=k):
                self.wait_recv(aa * z.I + lax.rem(b + k, z.I), c)

    def drain(self):
        @pl.loop(0, self.z.O)
        def _(aa):
            @pl.loop(0, self.pieces)
            def _(c):
                self.sends(aa, c, lambda copy: copy.wait_send())


class Reduce:
    def __init__(self, z, place, bufs, sems, piece, out, out_row):
        self.z, self.place, self.piece = z, place, piece
        self.stage, self.near, self.up, self.dn = bufs
        self.sx, self.rx, self.sz, self.ru, self.rd = sems
        self.out, self.out_row = out, out_row

    def rows(self, c):
        return pl.ds(c * self.z.P, self.z.P)

    def x_copy(self, aa, k, c):
        z, (a, b) = self.z, self.place
        at = aa * (z.I - 1) + k - 1
        return remote(
            self.stage.at[aa * z.I + lax.rem(b + k, z.I), self.rows(c)],
            self.near.at[at, self.rows(c)],
            self.sx.at[at * z.n + c],
            self.rx.at[at * z.n + c],
            "tensor",
            a * z.I + lax.rem(b + k, z.I),
        )

    def z_copy(self, aa, c, up):
        z, (a, b) = self.z, self.place
        box, sem = (self.up, self.ru) if up else (self.dn, self.rd)
        rank = lax.rem(a + (1 if up else z.O - 1), z.O) * z.I + b
        at = aa * z.n + c
        return remote(
            self.stage.at[aa * z.I + b, self.rows(c)],
            box.at[aa, self.rows(c)],
            self.sz.at[at],
            sem.at[at],
            "tensor",
            rank,
        )

    def produce(self, aa, k, term):
        z, (a, b) = self.z, self.place
        slot = aa * z.I + lax.rem(b + k, z.I)
        self.stage[slot] = term(slot).astype(bf16)
        if k:
            for c in range(z.n):
                self.x_copy(aa, k, c).start()

    def collect(self, aa):
        z, (a, b) = self.z, self.place

        @pl.loop(0, z.n)
        def _(c):
            rows = pl.ds(pl.multiple_of(c * z.P, 16), z.P)
            value = self.stage[aa * z.I + b, rows, :].astype(f32)
            for k in range(1, z.I):
                self.x_copy(aa, k, c).wait_recv()
                value += self.near[aa * (z.I - 1) + k - 1, rows, :].astype(f32)
            self.piece[...] = value

            @pl.when((aa >= a) & (a > 0))
            def _():
                self.z_copy(aa, c, True).wait_recv()
                self.piece[...] += self.up[aa, rows, :].astype(f32)

            @pl.when((aa <= a) & (a < z.O - 1))
            def _():
                self.z_copy(aa, c, False).wait_recv()
                self.piece[...] += self.dn[aa, rows, :].astype(f32)

            @pl.when(aa == a)
            def _():
                at = pl.ds(pl.multiple_of(self.out_row + c * z.P, 8), z.P)
                self.out[at, :] = self.piece[...]

            @pl.when(aa != a)
            def _():
                self.stage[aa * z.I + b, rows, :] = self.piece[...].astype(bf16)

            @pl.when(aa > a)
            def _():
                self.z_copy(aa, c, True).start()

            @pl.when(aa < a)
            def _():
                self.z_copy(aa, c, False).start()

    def drain(self):
        z, (a, b) = self.z, self.place

        @pl.loop(0, z.O)
        def _(aa):
            @pl.loop(0, z.n)
            def _(c):
                for k in range(1, z.I):
                    self.x_copy(aa, k, c).wait_send()

                @pl.when(aa != a)
                def _():
                    self.z_copy(aa, c, True).wait_send()


class Exchange:
    def __init__(self, axis, rank, count, box, own, send, recv):
        self.axis, self.rank, self.count, self.box, self.own = axis, rank, count, box, own
        self.send, self.recv = send, recv

    def copy(self, k):
        peer = lax.rem(self.rank + k, self.count)
        own = self.own.at[peer] if len(self.own.shape) == len(self.box.shape) else self.own
        return remote(
            own, self.box.at[self.rank], self.send.at[k], self.recv.at[self.rank], self.axis, peer
        )

    def start(self):
        for k in range(1, self.count):
            self.copy(k).start()

    def wait(self):
        for k in range(1, self.count):
            peer = lax.rem(self.rank + k, self.count)
            slot = self.box.at[peer]
            remote(slot, slot, self.send.at[k], self.recv.at[peer], self.axis, peer).wait_recv()

    def total(self):
        value = self.box[0].astype(f32)
        for k in range(1, self.count):
            value += self.box[k].astype(f32)
        return value

    def drain(self):
        for k in range(1, self.count):
            self.copy(k).wait_send()


def rope(x, cosine, sine):
    return x * cosine + pltpu.roll(x, HEAD_SIZE // 2, 1) * sine


def make_kernel(z, names, scratch):
    R, PW, T, D, O, I, C, Y = z.R, z.PW, z.T, z.D, z.O, z.I, z.C, z.Y
    L, S, QC, KC, NC, NW = z.L, z.S, z.QC, z.KC, z.NC, z.NW
    n_tile = pick(NW, (384, 512, 256, 128))

    def kernel(*refs):
        m = Refs()
        work = jax.tree.unflatten(jax.tree.structure(scratch), refs[len(names) :])
        for name, ref in [*zip(names, refs), *work.items()]:
            setattr(m, name, ref)
        t, d = lax.axis_index("tensor"), lax.axis_index("dp")
        a, b = lax.div(t, I), lax.rem(t, I)
        y, core = lax.div(d, C), lax.rem(d, C)
        place = (a, b)
        lane = lax.broadcasted_iota(jnp.int32, (1, LANES), 1)

        held, normed, W, WO, acc = m.held, m.normed, m.W, m.WO, m.acc

        def to_lanes(column):
            eye = lax.broadcasted_iota(jnp.int32, (R, z.Rp), 0) == lax.broadcasted_iota(
                jnp.int32, (R, z.Rp), 1
            )
            return jnp.sum(jnp.where(eye, column, 0.0), axis=0, keepdims=True)

        def to_column(row):
            eye = lax.broadcasted_iota(jnp.int32, (R, z.Rp), 0) == lax.broadcasted_iota(
                jnp.int32, (R, z.Rp), 1
            )
            return jnp.sum(jnp.where(eye, row, 0.0), axis=1, keepdims=True)

        def stack_rows(rows):
            index = lax.broadcasted_iota(jnp.int32, (8, z.Rp), 0)
            out = jnp.zeros((8, z.Rp), f32)
            for i, row in enumerate(rows):
                out = jnp.where(index == i, row, out)
            return out

        def chunks(fn, total=R):
            @pl.loop(0, total // z.step)
            def _(i):
                fn(pl.ds(pl.multiple_of(i * z.step, 16), z.step))

        def exchange(refs, count=T, axis="tensor", rank=t):
            return Exchange(axis, rank, count, *refs)

        loads = [
            (m.pol_hidden, held.at[t, pl.ds(0, R)]),
            (m.ref_hidden, held.at[t, pl.ds(R, R)]),
            (m.w_query, W.at[d, :, pl.ds(0, QC)]),
            (m.w_key, W.at[d, :, pl.ds(QC, KC)]),
            (m.value_projection, W.at[d, :, pl.ds(QC + KC, KC)]),
            (m.a_both, W.at[d, :, pl.ds(NC, z.AR)]),
            (m.w_out, WO.at[d]),
        ]
        copies = [
            pltpu.make_async_copy(src, dst, m.load[0].at[i]) for i, (src, dst) in enumerate(loads)
        ]
        for copy in copies:
            copy.start()

        barrier = pltpu.get_barrier_semaphore()
        for k in range(1, T):
            pl.semaphore_signal(
                barrier, inc=1, device_id={"tensor": lax.rem(t + k, T)}, device_id_type=MESH
            )
        for k in range(1, D):
            pl.semaphore_signal(
                barrier, inc=1, device_id={"dp": lax.rem(d + k, D)}, device_id_type=MESH
            )

        acc[...] = jnp.zeros_like(acc)
        m.F[...] = jnp.zeros_like(m.F)
        m.F[0 : z.rank, 0:QC] = m.query_second_factor[...]
        m.F[z.rank :, QC:] = m.value_second_factor[...]
        for s in range(S):
            slot = lax.broadcasted_iota(jnp.int32, (L, 1), 0)
            m.liv[s * L : (s + 1) * L, :] = (slot < m.lengths[s]).astype(f32)

        def square(rows):
            x = held[t, rows, :].astype(f32)
            m.col[rows, :] = jnp.sum(x * x, axis=1, keepdims=True)

        stats0 = exchange(m.s0)
        copies[0].wait()
        copies[1].wait()
        chunks(square, 2 * R)
        stats0.own[...] = stack_rows([to_lanes(m.col[0:R]), to_lanes(m.col[R:])])
        stats0.box[t] = stats0.own[...]
        pl.semaphore_wait(barrier, T - 1 + D - 1)
        stats0.start()

        hid = [Gather(z, place, held, m.hid[model], model * R) for model in range(2)]
        hid[0].start()
        hid[1].start()

        def weight_copy(job, slot, piece, k, far):
            buf, (recv, across, beside) = job
            block = buf.at[slot, pl.ds(piece * PW, PW)]
            if far:
                send = across.at[(k - 1) * z.r + piece]
                rank = lax.rem(y + k, Y) * C + core
            else:
                send = beside.at[(lax.div(slot, C) * (C - 1) + k - 1) * z.r + piece]
                rank = y * C + lax.rem(core + k, C)
            return remote(block, block, send, recv.at[slot * z.r + piece], "dp", rank)

        def order_of(q):
            return lax.rem(b + 1 + q, z.r)

        def weights_start(job):
            for q in range(z.r):
                for k in range(1, Y):
                    weight_copy(job, d, order_of(q), k, True).start()
                for k in range(1, C):
                    weight_copy(job, d, order_of(q), k, False).start()

        def weights_wait(job, slot, piece):
            weight_copy(job, slot, piece, 1, Y > 1).wait_recv()

        def weights_relay(job, q):
            for jj in range(1, Y):
                slot = lax.rem(y + jj, Y) * C + core
                weights_wait(job, slot, order_of(q))
                for k in range(1, C):
                    weight_copy(job, slot, order_of(q), k, False).start()

        def weights_wait_core(job, yy, q):
            for k in range(1, C):
                weights_wait(job, yy * C + lax.rem(core + k, C), order_of(q))

        def weights_drain(job):
            for q in range(z.r):
                for k in range(1, Y):
                    weight_copy(job, d, order_of(q), k, True).wait_send()
                for yy in range(Y):
                    for k in range(1, C):
                        weight_copy(job, yy * C + core, order_of(q), k, False).wait_send()

        wq, wo = (W, m.wq), (WO, m.wo)
        for copy in copies[2:6]:
            copy.wait()
        weights_start(wq)
        copies[6].wait()
        weights_start(wo)

        stats0.wait()

        scale = lax.rsqrt(stats0.total() / z.W + NORM_EPS)
        m.scol[0:R, :] = to_column(scale[0:1])
        m.scol[R:, :] = to_column(scale[1:2])

        def normalise(model, slot):
            gain = m.gains[pl.ds(slot, 1), :]

            def one(rows):
                at = pl.ds(pl.multiple_of(model * R + rows.start, 16), rows.size)
                x = held[slot, at, :].astype(f32)
                normed[slot, at, :] = (x * m.scol[at, :] * gain).astype(bf16)

            chunks(one)

        def arrive(model, aa):
            hid[model].wait_inner(aa)

            @pl.loop(0, I)
            def _(bb):
                normalise(model, aa * I + bb)

        def project(model, slot):
            row, count = model * R, R
            ws, off = lax.div(slot, z.r), lax.rem(slot, z.r) * PW

            @pl.loop(0, NW // n_tile)
            def _(i):
                cols = pl.ds(pl.multiple_of(i * n_tile, LANES), n_tile)
                acc[row : row + count, cols] += dot(
                    normed[slot, row : row + count, :],
                    W[ws, pl.ds(pl.multiple_of(off, 16), PW), cols],
                )

        def project_group(model, aa, stages):
            @pl.loop(0, I)
            def _(bb):
                slot = aa * I + bb
                near = lax.div(lax.div(slot, z.r), C) == y
                first = lax.rem(slot, z.r) != order_of(z.r - 1)
                kinds = [
                    near,
                    jnp.logical_not(near) & first,
                    jnp.logical_not(near) & jnp.logical_not(first),
                ]
                wanted = kinds[stages[0]]
                for stage in stages[1:]:
                    wanted = wanted | kinds[stage]

                @pl.when(wanted)
                def _():
                    project(model, slot)

        side = jnp.minimum(a, O - 1 - a)

        def visit(j):
            inside = jnp.where(lax.rem(j, 2) == 1, a - lax.div(j + 1, 2), a + lax.div(j, 2))
            outside = jnp.where(a <= O - 1 - a, a + j - side, a - j + side)
            return jnp.where(j <= 2 * side, inside, outside)

        for q in range(z.r):
            weights_wait_core(wq, y, q)

        @pl.loop(1, O)
        def _(j):
            hid[0].relay(visit(j))
            arrive(0, visit(j - 1))
            project_group(0, visit(j - 1), [0])

        for q in range(z.r - 1):
            weights_relay(wq, q)
            for jj in range(1, Y):
                weights_wait_core(wq, lax.rem(y + jj, Y), q)

        @pl.loop(1, O)
        def _(j):
            hid[1].relay(visit(j))

        arrive(0, visit(O - 1))
        project_group(0, visit(O - 1), [0])

        @pl.loop(0, O)
        def _(j):
            project_group(0, j, [1])

        @pl.loop(0, O - 1)
        def _(j):
            arrive(1, visit(j))
            project_group(1, visit(j), [0, 1])

        weights_relay(wq, z.r - 1)
        for jj in range(1, Y):
            weights_wait_core(wq, lax.rem(y + jj, Y), z.r - 1)

        @pl.loop(0, O)
        def _(j):
            project_group(0, j, [2])

        row_slot = lax.broadcasted_iota(jnp.int32, (L, L), 0)
        key_slot = lax.broadcasted_iota(jnp.int32, (L, L), 1)
        causal = key_slot <= row_slot

        def attend(model):
            base = model * R
            if model == 0:
                m.low[...] = acc[0:R, NC:NW].astype(bf16)
                m.added[...] = ADAPTER_SCALE * dot(m.low[...], m.F[...])

            @pl.loop(0, S)
            def _(s):
                rows = pl.ds(pl.multiple_of(base + s * L, 16), L)
                local = pl.ds(pl.multiple_of(s * L, 16), L)
                allowed = causal & (key_slot < m.lengths[s])
                allowed = jnp.concatenate([allowed.astype(f32)] * z.G, axis=0) > 0.5
                cosine, sine = m.cosine[...], m.sine[...]
                for k in range(z.KV):
                    head = slice(k * HEAD_SIZE, (k + 1) * HEAD_SIZE)
                    kh = acc[rows, QC + k * HEAD_SIZE : QC + (k + 1) * HEAD_SIZE]
                    vh = acc[rows, QC + KC + k * HEAD_SIZE : QC + KC + (k + 1) * HEAD_SIZE]
                    if model == 0:
                        vh = vh + m.added[local, QC + k * HEAD_SIZE : QC + (k + 1) * HEAD_SIZE]
                    kh = rope(kh, cosine, sine).astype(bf16)
                    vh = vh.astype(bf16)
                    queries = []
                    for g in range(z.G):
                        h = k * z.G + g
                        qh = acc[rows, h * HEAD_SIZE : (h + 1) * HEAD_SIZE]
                        if model == 0:
                            qh = qh + m.added[local, h * HEAD_SIZE : (h + 1) * HEAD_SIZE]
                        queries.append(rope(qh, cosine, sine).astype(bf16))
                    q2 = jnp.concatenate(queries, axis=0)
                    scores = dot(q2, kh, NT) * query_scale()
                    capped = SOFT_CAP * jnp.tanh(scores / SOFT_CAP)
                    weights = jnp.where(allowed, jnp.exp(capped), 0.0)
                    probs = weights / jnp.sum(weights, axis=1, keepdims=True)
                    out = dot(probs.astype(bf16), vh).astype(bf16)
                    for g in range(z.G):
                        h = k * z.G + g
                        m.mixed[rows, h * HEAD_SIZE : (h + 1) * HEAD_SIZE] = out[
                            g * L : (g + 1) * L
                        ]
                    if model == 0:
                        m.q2[s, k] = q2
                        m.kk[s, k] = kh
                        m.vv[s, k] = vh
                        m.probs[s, k] = probs
                        m.capped[s, k] = capped

        attend(0)

        def out_term(model):
            def term(slot):
                ws, off = lax.div(slot, z.r), lax.rem(slot, z.r) * PW
                return dot(
                    m.mixed[model * R : (model + 1) * R, :],
                    WO[ws, pl.ds(pl.multiple_of(off, 16), PW), :],
                    NT,
                )

            return term

        def reduce_of(bufs, sems, out, row):
            return Reduce(
                z,
                place,
                bufs,
                sems,
                m.piece,
                out,
                row,
            )

        red_pol = reduce_of(m.pol, m.pol_sems, m.summed, 0)
        red_ref = reduce_of(m.ref, m.ref_sems, m.summed, R)
        red_grad = reduce_of(m.pol, m.grad_sems, m.gnorm, 0)

        def near_first(j):
            yy, jj = lax.rem(y + lax.div(j, z.gp), Y), lax.rem(j, z.gp)
            low = yy * z.gp + jj
            high = yy * z.gp + z.gp - 1 - jj
            return jnp.where(2 * yy < Y, low, high)

        def far_first(j):
            return visit(O - 1 - j)

        def produce_range(red, first, last, order, term, ks):
            @pl.loop(first, last)
            def _(j):
                for k in ks:
                    red.produce(order(j), k, term)

        def collect_range(red, first, last, order):
            @pl.loop(first, last)
            def _(j):
                @pl.when(order(j) != a)
                def _():
                    red.collect(order(j))

        xs, own = list(range(1, I)), [0]
        for q in range(z.r):
            weights_wait_core(wo, y, q)
        produce_range(red_pol, 0, z.gp, near_first, out_term(0), xs + own)

        arrive(1, visit(O - 1))
        project_group(1, visit(O - 1), [0, 1])

        @pl.loop(0, O)
        def _(j):
            project_group(1, j, [2])

        attend(1)
        collect_range(red_pol, 0, z.gp, near_first)
        early = z.r if I != z.r else z.r - 1
        for q in range(early):
            weights_relay(wo, q)
            for jj in range(1, Y):
                weights_wait_core(wo, lax.rem(y + jj, Y), q)
        produce_range(red_pol, z.gp, O, near_first, out_term(0), xs)
        for q in range(early, z.r):
            weights_relay(wo, q)
            for jj in range(1, Y):
                weights_wait_core(wo, lax.rem(y + jj, Y), q)
        produce_range(red_pol, z.gp, O, near_first, out_term(0), own)
        produce_range(red_ref, 0, 1, far_first, out_term(1), xs + own)
        collect_range(red_pol, z.gp, O, near_first)
        produce_range(red_ref, 1, 2, far_first, out_term(1), xs + own)
        red_pol.collect(a)

        post_gain = m.gains[pl.ds(T + t, 1), :]

        def token_sums(model, refs):
            base = model * R

            def one(rows):
                at = pl.ds(base + rows.start, rows.size)
                x = m.summed[at, :]
                read = m.readout[rows, :].astype(f32)
                m.pcol[pl.ds(rows.start, rows.size), :] = jnp.sum(x * x, axis=1, keepdims=True)
                m.pcol[pl.ds(R + rows.start, rows.size), :] = jnp.sum(
                    x * (post_gain * read), axis=1, keepdims=True
                )
                h = held[t, at, :].astype(f32)
                m.pcol[pl.ds(2 * R + rows.start, rows.size), :] = jnp.sum(
                    h * read, axis=1, keepdims=True
                )

            chunks(one)
            done = exchange(refs)
            done.own[...] = stack_rows([to_lanes(m.pcol[i * R : (i + 1) * R]) for i in range(3)])
            done.box[t] = done.own[...]
            done.start()
            return done

        stats1 = token_sums(0, m.s1)
        produce_range(red_ref, 2, O, far_first, out_term(1), xs + own)
        stats1.wait()
        sums1 = stats1.total()
        post1 = lax.rsqrt(sums1[0:1] / z.W + NORM_EPS)
        m.col[0:R, :] = to_column(post1)
        m.col[R:, :] = to_column(post1 * post1 * post1 * sums1[1:2] / z.W)

        def make_grad(rows):
            read = m.readout[rows, :].astype(f32)
            value = m.col[rows, :] * post_gain * read - m.summed[rows, :] * m.col[
                pl.ds(R + rows.start, rows.size), :
            ]
            m.gheld[t, rows, :] = (value * m.liv[rows, :]).astype(bf16)

        chunks(make_grad)
        gag = Gather(z, place, m.gheld, m.gag)
        gag.start()

        def finish(model, out):
            def one(rows):
                at = pl.ds(model * R + rows.start, rows.size)
                h = held[t, at, :].astype(f32)
                out[rows, :] = (h + m.summed[at, :] * m.pcol[rows, :] * post_gain).astype(
                    bf16
                )

            chunks(one)

        m.pcol[0:R, :] = m.col[0:R, :]
        finish(0, m.policy_out)
        m.gm[...] = jnp.zeros_like(m.gm)

        def back_out(aa):
            @pl.loop(0, I)
            def _(bb):
                slot = aa * I + bb
                ws, off = lax.div(slot, z.r), lax.rem(slot, z.r) * PW
                m.gm[...] += dot(
                    m.gheld[slot], WO[ws, pl.ds(pl.multiple_of(off, 16), PW), :]
                )

        collect_range(red_ref, 0, O - 1, far_first)

        @pl.loop(1, O)
        def _(j):
            gag.relay(visit(j))

            @pl.when(j == O - 1)
            def _():
                red_ref.collect(a)

            gag.wait_inner(visit(j - 1))
            back_out(visit(j - 1))

        stats2 = token_sums(1, m.s2)
        gag.wait_inner(visit(O - 1))
        back_out(visit(O - 1))
        stats2.wait()
        sums2 = stats2.total()
        post2 = lax.rsqrt(sums2[0:1] / z.W + NORM_EPS)

        token_pol = sums1[2:3] + post1 * sums1[1:2]
        token_ref = sums2[2:3] + post2 * sums2[1:2]
        wide = lax.broadcasted_iota(jnp.int32, (1, z.Rp), 1)
        mine = jnp.zeros((1, LANES), f32)
        for s in range(S):
            inside = (wide >= s * L) & (wide < s * L + m.lengths[s])
            value = jnp.sum(jnp.where(inside, token_pol, 0.0), axis=1, keepdims=True) - jnp.sum(
                jnp.where(inside, token_ref, 0.0), axis=1, keepdims=True
            )
            mine = jnp.where(lane == d * S + s, value, mine)
        scores = exchange(m.score, D, "dp", d)
        scores.own[...] = jnp.broadcast_to(mine, (8, LANES))
        scores.box[d] = scores.own[...]
        scores.start()
        m.gmb[...] = m.gm[...].astype(bf16)

        @pl.loop(0, S)
        def _(s):
            rows = pl.ds(pl.multiple_of(s * L, 16), L)
            cosine, sine = m.cosine[...], -m.sine[...]
            for k in range(z.KV):
                parts = []
                for g in range(z.G):
                    h = k * z.G + g
                    parts.append(m.gmb[rows, h * HEAD_SIZE : (h + 1) * HEAD_SIZE])
                grad = jnp.concatenate(parts, axis=0)
                probs, capped = m.probs[s, k], m.capped[s, k]
                grad_probs = dot(grad, m.vv[s, k], NT)
                grad_v = dot(probs.astype(bf16), grad, TN)
                centered = grad_probs - jnp.sum(grad_probs * probs, axis=1, keepdims=True)
                ratio = capped / SOFT_CAP
                grad_scores = (
                    probs * centered * (1.0 - ratio * ratio) * query_scale()
                ).astype(bf16)
                grad_q = dot(grad_scores, m.kk[s, k])
                grad_k = dot(grad_scores, m.q2[s, k], TN)
                for g in range(z.G):
                    h = k * z.G + g
                    m.dcat[rows, h * HEAD_SIZE : (h + 1) * HEAD_SIZE] = rope(
                        grad_q[g * L : (g + 1) * L], cosine, sine
                    ).astype(bf16)
                at = QC + k * HEAD_SIZE
                m.dcat[rows, at : at + HEAD_SIZE] = rope(grad_k, cosine, sine).astype(bf16)
                m.dcat[rows, at + KC : at + KC + HEAD_SIZE] = grad_v.astype(bf16)

        m.dcat[:, NC:NW] = (
            ADAPTER_SCALE
            * (
                dot(m.dcat[:, 0:QC], m.F[:, 0:QC], NT)
                + dot(m.dcat[:, QC + KC : NC], m.F[:, QC:], NT)
            )
        ).astype(bf16)

        def in_term(slot):
            ws, off = lax.div(slot, z.r), lax.rem(slot, z.r) * PW
            return dot(m.dcat[...], W[ws, pl.ds(pl.multiple_of(off, 16), PW), :], NT)

        def pre_dot(rows):
            m.pcol[pl.ds(3 * R + rows.start, rows.size), :] = jnp.sum(
                m.dcat[rows, :].astype(f32) * acc[rows, :], axis=1, keepdims=True
            )

        def hook_part(part, k):
            return remote(
                m.dcat.at[pl.ds(pl.multiple_of(part * z.HR, 16), z.HR), pl.ds(NC, z.AR)],
                m.hbox.at[t],
                m.h1[0].at[k],
                m.h1[1].at[t],
                "tensor",
                lax.rem(t + k, T),
            )

        def hook_whole(k):
            mine = m.hsum.at[t]
            peer = lax.rem(t + k, T)
            return remote(mine, mine, m.h2[0].at[k], m.h2[1].at[t], "tensor", peer)

        for k in range(1, T):
            peer = lax.rem(t + k, T)

            @pl.when(peer < z.HN)
            def _(peer=peer, k=k):
                hook_part(peer, k).start()

        chunks(pre_dot)
        stats3 = exchange(m.s3)
        stats3.own[...] = stack_rows([to_lanes(m.pcol[3 * R :])])
        stats3.box[t] = stats3.own[...]
        stats3.start()
        red_pol.drain()
        produce_range(red_grad, 0, 1, far_first, in_term, xs + own)

        @pl.when(t < z.HN)
        def _():
            at = pl.ds(pl.multiple_of(t * z.HR, 16), z.HR)
            m.hbox[t] = m.dcat[at, NC:NW]
            for k in range(1, T):
                peer = lax.rem(t + k, T)
                slot = m.hbox.at[peer]
                remote(slot, slot, m.h1[0].at[k], m.h1[1].at[peer], "tensor", peer).wait_recv()
            value = m.hbox[0].astype(f32)
            for k in range(1, T):
                value += m.hbox[k].astype(f32)
            m.hsum[t] = value.astype(bf16)
            for k in range(1, T):
                hook_whole(k).start()

        produce_range(red_grad, 1, O, far_first, in_term, xs + own)
        scores.wait()
        ratios = scores.total()[0:1]
        loss = jnp.zeros((1, 1), f32)
        coefficients = jnp.zeros((1, LANES), f32)
        for k in range(S * D // 2):
            chosen, rejected = m.pairing[2 * k], m.pairing[2 * k + 1]
            margin = DPO_BETA * (
                jnp.sum(jnp.where(lane == chosen, ratios, 0.0), axis=1, keepdims=True)
                - jnp.sum(jnp.where(lane == rejected, ratios, 0.0), axis=1, keepdims=True)
            )
            soft = jnp.exp(-jnp.abs(margin))
            loss += jnp.maximum(-margin, 0.0) + jnp.log1p(soft)
            sigmoid = jnp.where(margin > 0, soft, 1.0) / (1.0 + soft)
            pull = DPO_BETA * LOSS_SCALE * sigmoid
            coefficients += jnp.where(lane == rejected, pull, 0.0) - jnp.where(
                lane == chosen, pull, 0.0
            )
        m.dpo_loss[...] = jnp.broadcast_to(loss, (8, LANES))
        own_coef = []
        for s in range(S):
            value = jnp.sum(jnp.where(lane == d * S + s, coefficients, 0.0), axis=1, keepdims=True)
            own_coef.append(value)
            m.ccol[s * L : (s + 1) * L, :] = jnp.broadcast_to(value, (L, 1))

        parts_q = jnp.zeros((z.rank, QC), f32)
        parts_v = jnp.zeros((z.rank, KC), f32)
        for s in range(S):
            rows = slice(s * L, (s + 1) * L)
            low = m.low[rows, :]
            parts_q += own_coef[s] * dot(low, m.dcat[rows, 0:QC], TN)[0 : z.rank]
            parts_v += own_coef[s] * dot(low, m.dcat[rows, QC + KC : NC], TN)[z.rank :]
        factors = exchange(m.fac, D, "dp", d)
        factors.own[:, 0:QC] = (ADAPTER_SCALE * parts_q).astype(bf16)
        factors.own[:, QC:] = (ADAPTER_SCALE * parts_v).astype(bf16)
        factors.box[d] = factors.own[...]
        factors.start()
        collect_range(red_grad, 0, 1, far_first)

        for k in range(1, T):
            peer = lax.rem(t + k, T)

            @pl.when(peer < z.HN)
            def _(peer=peer, k=k):
                slot = m.hsum.at[peer]
                remote(slot, slot, m.h2[0].at[k], m.h2[1].at[peer], "tensor", peer).wait_recv()

        hook = m.hsum[...].reshape(R, z.AR)
        hook = (hook.astype(f32) * m.ccol[...]).astype(bf16)
        adapters = exchange(m.ad, D, "dp", d)

        @pl.loop(0, T)
        def _(slot):
            ws, off = lax.div(slot, z.r), lax.rem(slot, z.r) * PW
            adapters.own[ws, pl.ds(pl.multiple_of(off, 16), PW), :] = dot(
                normed[slot, 0:R, :], hook, TN
            ).astype(bf16)

        adapters.box[d] = adapters.own[d]
        adapters.start()
        collect_range(red_grad, 1, O, far_first)
        m.pcol[0:R, :] = to_column(post2)
        finish(1, m.reference_out)
        stats3.wait()
        m.pcol[0:R, :] = to_column(stats3.total()[0:1])
        factors.wait()
        value = factors.total()
        m.query_factor_gradient[...] = value[:, 0:QC]
        m.value_factor_gradient[...] = value[:, QC:]
        red_grad.collect(a)

        pre_gain = m.gains[pl.ds(t, 1), :]

        def grad_in(rows):
            read = m.readout[rows, :].astype(f32) * m.liv[rows, :]
            scale = m.scol[rows, :]
            h = held[t, rows, :].astype(f32)
            value = (
                read
                + scale * pre_gain * m.gnorm[rows, :]
                - h * (scale * scale * m.pcol[rows, :] / z.W)
            )
            m.grad_hidden[rows, :] = (value * m.ccol[rows, :]).astype(bf16)

        chunks(grad_in)
        adapters.wait()

        def sum_adapters(rows):
            value = adapters.box[0, rows, :].astype(f32)
            for k in range(1, D):
                value += adapters.box[k, rows, :].astype(f32)
            m.grad_a[rows, :] = value

        size = pick(z.r * PW, (96, 48, 32, 16))

        @pl.loop(0, z.r * PW // size)
        def _(i):
            sum_adapters(pl.ds(pl.multiple_of(i * size, 16), size))

        hid[0].drain()
        hid[1].drain()
        gag.drain()
        red_ref.drain()
        red_grad.drain()
        weights_drain(wq)
        weights_drain(wo)
        for done in (stats0, stats1, stats2, stats3, scores, factors, adapters):
            done.drain()
        for k in range(1, T):
            peer = lax.rem(t + k, T)

            @pl.when(peer < z.HN)
            def _(peer=peer, k=k):
                hook_part(peer, k).wait_send()

        @pl.when(t < z.HN)
        def _():
            for k in range(1, T):
                hook_whole(k).wait_send()

    return kernel


def body(
    ref_hidden,
    pol_hidden,
    readout,
    lengths,
    pairing,
    pre_gain,
    post_gain,
    w_query,
    w_key,
    value_projection,
    w_out,
    a_query,
    a_value,
    query_second_factor,
    value_second_factor,
):
    z = Sizes(
        pol_hidden.shape[0],
        pol_hidden.shape[1],
        lengths.shape[0],
        lax.axis_size("dp"),
        lax.axis_size("tensor"),
        w_query.shape[1],
        w_key.shape[1],
        query_second_factor.shape[0],
    )
    gains = jnp.concatenate([pre_gain.reshape(z.T, z.PW), post_gain.reshape(z.T, z.PW)], axis=0)
    a_both = jnp.concatenate([a_query, a_value], axis=1)
    cosine, sine = rope_tables(z.L)
    vmem = pl.BlockSpec(memory_space=pltpu.VMEM)
    smem = pl.BlockSpec(memory_space=pltpu.SMEM)
    hbm = pl.BlockSpec(memory_space=pl.ANY)
    inputs = dict(
        pol_hidden=(pol_hidden, hbm),
        ref_hidden=(ref_hidden, hbm),
        readout=(readout, vmem),
        lengths=(lengths, smem),
        pairing=(pairing, smem),
        gains=(gains, vmem),
        w_query=(w_query, hbm),
        w_key=(w_key, hbm),
        value_projection=(value_projection, hbm),
        w_out=(w_out, hbm),
        a_both=(a_both, hbm),
        query_second_factor=(query_second_factor, vmem),
        value_second_factor=(value_second_factor, vmem),
        cosine=(jnp.asarray(cosine), vmem),
        sine=(jnp.asarray(sine), vmem),
    )
    outputs = dict(
        policy_out=((z.R, z.PW), bf16),
        reference_out=((z.R, z.PW), bf16),
        dpo_loss=((8, LANES), f32),
        grad_hidden=((z.R, z.PW), bf16),
        grad_a=((z.r * z.PW, z.AR), f32),
        query_factor_gradient=((z.rank, z.QC), f32),
        value_factor_gradient=((z.rank, z.KC), f32),
    )
    scratch = build_scratch(z)
    outs = pl.pallas_call(
        make_kernel(z, [*inputs, *outputs], scratch),
        name="preference_step",
        out_shape=[jax.ShapeDtypeStruct(*entry) for entry in outputs.values()],
        in_specs=[spec for _, spec in inputs.values()],
        out_specs=[vmem] * len(outputs),
        scratch_shapes=jax.tree.leaves(scratch),
        compiler_params=pltpu.CompilerParams(
            collective_id=1, has_side_effects=True, vmem_limit_bytes=VMEM_GRANT
        ),
    )(*[array for array, _ in inputs.values()])
    policy_out, reference_out, loss, grad_hidden, grad_a, grad_q, grad_v = outs
    return policy_out, reference_out, loss[0, 0], grad_hidden, grad_a, grad_q, grad_v


def solution(mesh):
    placed = (
        P("dp", "tensor"),
        P("dp", "tensor"),
        P("dp", "tensor"),
        P("dp"),
        P(),
        P(),
        P(),
        P("dp", "tensor"),
        P("dp", "tensor"),
        P("dp", "tensor"),
        P("dp", "tensor"),
        P("dp", None),
        P("dp", None),
        P(None, "tensor"),
        P(None, "tensor"),
    )
    return jax.shard_map(
        body,
        mesh=mesh,
        in_specs=placed,
        out_specs=(
            P("dp", "tensor"),
            P("dp", "tensor"),
            P(),
            P("dp", "tensor"),
            P("dp", None),
            P(None, "tensor"),
            P(None, "tensor"),
        ),
        check_vma=False,
    )
```

```python
import jax
import jax.numpy as jnp
import numpy as np
from jax import lax
from jax.experimental import pallas as pl
from jax.experimental.pallas import tpu as pltpu
from jax.sharding import PartitionSpec as P

MODEL_WIDTH = 4608
HQ = 32
HEAD_SIZE = 128


NORM_EPS = 1e-06
SOFT_CAP = 50.0
ADAPTER_SCALE = 0.5
DPO_BETA = 0.5
LOSS_SCALE = 256.0
ROPE_BASE = 10000.0

MESH = pl.DeviceIdType.MESH
VMEM_GRANT = 67_000_000
LANES = 128
f32, bf16 = jnp.float32, jnp.bfloat16
NT = (((1,), (1,)), ((), ()))
TN = (((0,), (0,)), ((), ()))


def query_scale():
    return float(MODEL_WIDTH // HQ) ** (-0.5)


def grid_of(axis, count):
    if axis == "dp":
        inner = 2 if count % 2 == 0 else 1
    else:
        inner = 1
        while (inner * 2) ** 2 <= count and count % (inner * 2) == 0:
            inner *= 2
    return count // inner, inner


def pick(size, options):
    for option in options:
        if size % option == 0:
            return option
    return size


def rope_tables(length):
    half = HEAD_SIZE // 2
    spacing = ROPE_BASE ** (-2.0 * np.arange(half, dtype=np.float32) / HEAD_SIZE)
    angles = np.arange(length, dtype=np.float32)[:, None] * spacing[None, :].astype(np.float32)
    cosine, sine = np.cos(angles), np.sin(angles)
    return (
        np.concatenate([cosine, cosine], axis=1).astype(np.float32),
        np.concatenate([-sine, sine], axis=1).astype(np.float32),
    )


def dot(x, y, dims=(((1,), (0,)), ((), ()))):
    return lax.dot_general(x, y, dims, preferred_element_type=f32)


def remote(src, dst, send_sem, recv_sem, axis, rank):
    return pltpu.make_async_remote_copy(
        src_ref=src,
        dst_ref=dst,
        send_sem=send_sem,
        recv_sem=recv_sem,
        device_id={axis: rank},
        device_id_type=MESH,
    )


class Sizes:
    def __init__(self, tok_rows, part_width, seqs, dp, tensor, q_cols, k_cols, rank):
        self.R, self.PW, self.S, self.D, self.T = tok_rows, part_width, seqs, dp, tensor
        self.L = tok_rows // seqs
        self.QC, self.KC = q_cols, k_cols
        self.AR = 2 * rank
        self.rank = rank
        self.NC = q_cols + 2 * k_cols
        self.NW = self.NC + self.AR
        self.O, self.I = grid_of("tensor", tensor)
        self.Y, self.C = grid_of("dp", dp)
        self.r = tensor // dp
        self.gp = max(self.O // self.Y, 1)
        self.KV = k_cols // HEAD_SIZE
        self.G = q_cols // k_cols
        self.P = self.L
        self.n = tok_rows // self.P
        self.Rp = -(-tok_rows // LANES) * LANES
        self.W = part_width * tensor
        self.step = pick(tok_rows, (48, 32, 16))
        size = 16
        while tok_rows % size or tok_rows // size > tensor:
            size += 16
        self.HR, self.HN = size, tok_rows // size


def vm(*shape, kind=bf16):
    return pltpu.VMEM(shape, kind)


def sem(*counts):
    return [pltpu.SemaphoreType.DMA((max(count, 1),)) for count in counts]


def build_scratch(z):
    R, PW, T, D, O, I, n = z.R, z.PW, z.T, z.D, z.O, z.I, z.n
    inner = O * (I - 1)
    moved = z.QC + z.KC

    def boxes():
        return [vm(T, R, PW), vm(max(inner, 1), R, PW), vm(O, R, PW), vm(O, R, PW)]

    def reduce_sems():
        return sem(inner * n, inner * n, O * n, O * n, O * n)

    def gather_sems(count):
        return sem(T * count, O * count, O * count, inner * count)

    def stat():
        return [vm(T, 8, z.Rp, kind=f32), vm(8, z.Rp, kind=f32)] + sem(T, T)

    def weight_sems():
        return sem(D * z.r, (z.Y - 1) * z.r, z.Y * (z.C - 1) * z.r)

    return dict(
        held=vm(T, 2 * R, PW),
        normed=vm(T, 2 * R, PW),
        W=vm(D, z.r * PW, z.NW),
        WO=vm(D, z.r * PW, z.QC),
        acc=vm(2 * R, z.NW, kind=f32),
        added=vm(R, moved, kind=f32),
        low=vm(R, z.AR),
        F=vm(z.AR, moved),
        q2=vm(z.S, z.KV, z.G * z.L, HEAD_SIZE),
        kk=vm(z.S, z.KV, z.L, HEAD_SIZE),
        vv=vm(z.S, z.KV, z.L, HEAD_SIZE),
        probs=vm(z.S, z.KV, z.G * z.L, z.L, kind=f32),
        capped=vm(z.S, z.KV, z.G * z.L, z.L, kind=f32),
        mixed=vm(2 * R, z.QC),
        pol=boxes(),
        ref=boxes(),
        pol_sems=reduce_sems(),
        ref_sems=reduce_sems(),
        grad_sems=reduce_sems(),
        piece=vm(z.P, PW, kind=f32),
        summed=vm(2 * R, PW, kind=f32),
        gheld=vm(T, R, PW),
        gm=vm(R, z.QC, kind=f32),
        gmb=vm(R, z.QC),
        dcat=vm(R, z.NW),
        gnorm=vm(R, PW, kind=f32),
        col=vm(2 * R, 1, kind=f32),
        scol=vm(2 * R, 1, kind=f32),
        liv=vm(R, 1, kind=f32),
        ccol=vm(R, 1, kind=f32),
        pcol=vm(4 * R, 1, kind=f32),
        s0=stat(),
        s1=stat(),
        s2=stat(),
        s3=stat(),
        score=[vm(D, 8, LANES, kind=f32), vm(8, LANES, kind=f32)] + sem(D, D),
        hbox=vm(T, z.HR, z.AR),
        hsum=vm(z.HN, z.HR, z.AR),
        h1=sem(T, T),
        h2=sem(T, T),
        fac=[vm(D, z.rank, moved), vm(z.rank, moved)] + sem(D, D),
        ad=[vm(D, z.r * PW, z.AR), vm(D, z.r * PW, z.AR)] + sem(D, D),
        load=sem(16),
        emit=sem(8),
        a_in=vm(2, z.r * PW, z.rank),
        query_second_factor=vm(z.rank, z.QC),
        value_second_factor=vm(z.rank, z.KC),
        gains=vm(2 * T, PW, kind=f32),
        readout=vm(R, PW),
        cosine=vm(z.L, HEAD_SIZE, kind=f32),
        sine=vm(z.L, HEAD_SIZE, kind=f32),
        policy_out=vm(R, PW),
        reference_out=vm(R, PW),
        dpo_loss=vm(8, LANES, kind=f32),
        grad_hidden=vm(R, PW),
        grad_a=vm(z.r * PW, z.AR, kind=f32),
        query_factor_gradient=vm(z.rank, z.QC, kind=f32),
        value_factor_gradient=vm(z.rank, z.KC, kind=f32),
        hid=[gather_sems(n), gather_sems(n)],
        gag=gather_sems(n),
        wq=weight_sems(),
        wo=weight_sems(),
    )


class Refs:
    pass


class Gather:
    def __init__(self, z, place, held, sems, row=0):
        self.z, self.place, self.held, self.pieces = z, place, held, z.n
        self.r, self.u, self.d, self.x = sems
        self.row = row

    def block(self, slot, c):
        return self.held.at[slot, pl.ds(self.row + c * self.z.P, self.z.P)]

    def copy(self, aa, c, kind, k=0):
        z, (a, b) = self.z, self.place
        slot = aa * z.I + b
        block = self.block(slot, c)
        at = aa * self.pieces + c
        if kind == "up":
            send, rank = self.u.at[at], lax.rem(a + 1, z.O) * z.I + b
        elif kind == "dn":
            send, rank = self.d.at[at], lax.rem(a + z.O - 1, z.O) * z.I + b
        else:
            send = self.x.at[(aa * (z.I - 1) + k - 1) * self.pieces + c]
            rank = a * z.I + lax.rem(b + k, z.I)
        return remote(block, block, send, self.r.at[slot * self.pieces + c], "tensor", rank)

    def wait_recv(self, slot, c):
        z = self.z
        block = self.block(slot, c)
        at = slot * self.pieces + c
        remote(block, block, self.u.at[0], self.r.at[at], "tensor", 0).wait_recv()

    def sends(self, aa, c, act):
        z, (a, b) = self.z, self.place

        @pl.when((aa <= a) & (a < z.O - 1))
        def _():
            act(self.copy(aa, c, "up"))

        @pl.when((aa >= a) & (a > 0))
        def _():
            act(self.copy(aa, c, "dn"))

        for k in range(1, z.I):
            act(self.copy(aa, c, "x", k))

    def start(self):
        for c in range(self.pieces):
            self.sends(self.place[0], c, lambda copy: copy.start())

    def relay(self, aa):
        z, (a, b) = self.z, self.place

        @pl.loop(0, self.pieces)
        def _(c):
            self.wait_recv(aa * z.I + b, c)
            self.sends(aa, c, lambda copy: copy.start())

    def wait_inner(self, aa):
        z, (a, b) = self.z, self.place
        for k in range(1, z.I):

            @pl.loop(0, self.pieces)
            def _(c, k=k):
                self.wait_recv(aa * z.I + lax.rem(b + k, z.I), c)

    def drain(self):
        @pl.loop(0, self.z.O)
        def _(aa):
            @pl.loop(0, self.pieces)
            def _(c):
                self.sends(aa, c, lambda copy: copy.wait_send())


class Reduce:
    def __init__(self, z, place, bufs, sems, piece, out, out_row):
        self.z, self.place, self.piece = z, place, piece
        self.stage, self.near, self.up, self.dn = bufs
        self.sx, self.rx, self.sz, self.ru, self.rd = sems
        self.out, self.out_row = out, out_row

    def rows(self, c):
        return pl.ds(c * self.z.P, self.z.P)

    def x_copy(self, aa, k, c):
        z, (a, b) = self.z, self.place
        at = aa * (z.I - 1) + k - 1
        return remote(
            self.stage.at[aa * z.I + lax.rem(b + k, z.I), self.rows(c)],
            self.near.at[at, self.rows(c)],
            self.sx.at[at * z.n + c],
            self.rx.at[at * z.n + c],
            "tensor",
            a * z.I + lax.rem(b + k, z.I),
        )

    def z_copy(self, aa, c, up):
        z, (a, b) = self.z, self.place
        box, sem = (self.up, self.ru) if up else (self.dn, self.rd)
        rank = lax.rem(a + (1 if up else z.O - 1), z.O) * z.I + b
        at = aa * z.n + c
        return remote(
            self.stage.at[aa * z.I + b, self.rows(c)],
            box.at[aa, self.rows(c)],
            self.sz.at[at],
            sem.at[at],
            "tensor",
            rank,
        )

    def produce(self, aa, k, term):
        z, (a, b) = self.z, self.place
        slot = aa * z.I + lax.rem(b + k, z.I)
        self.stage[slot] = term(slot).astype(bf16)
        if k:
            for c in range(z.n):
                self.x_copy(aa, k, c).start()

    def collect(self, aa):
        z, (a, b) = self.z, self.place

        @pl.loop(0, z.n)
        def _(c):
            rows = pl.ds(pl.multiple_of(c * z.P, 16), z.P)
            value = self.stage[aa * z.I + b, rows, :].astype(f32)
            for k in range(1, z.I):
                self.x_copy(aa, k, c).wait_recv()
                value += self.near[aa * (z.I - 1) + k - 1, rows, :].astype(f32)
            self.piece[...] = value

            @pl.when((aa >= a) & (a > 0))
            def _():
                self.z_copy(aa, c, True).wait_recv()
                self.piece[...] += self.up[aa, rows, :].astype(f32)

            @pl.when((aa <= a) & (a < z.O - 1))
            def _():
                self.z_copy(aa, c, False).wait_recv()
                self.piece[...] += self.dn[aa, rows, :].astype(f32)

            @pl.when(aa == a)
            def _():
                at = pl.ds(pl.multiple_of(self.out_row + c * z.P, 8), z.P)
                self.out[at, :] = self.piece[...]

            @pl.when(aa != a)
            def _():
                self.stage[aa * z.I + b, rows, :] = self.piece[...].astype(bf16)

            @pl.when(aa > a)
            def _():
                self.z_copy(aa, c, True).start()

            @pl.when(aa < a)
            def _():
                self.z_copy(aa, c, False).start()

    def drain(self):
        z, (a, b) = self.z, self.place

        @pl.loop(0, z.O)
        def _(aa):
            @pl.loop(0, z.n)
            def _(c):
                for k in range(1, z.I):
                    self.x_copy(aa, k, c).wait_send()

                @pl.when(aa != a)
                def _():
                    self.z_copy(aa, c, True).wait_send()


class Exchange:
    def __init__(self, axis, rank, count, box, own, send, recv):
        self.axis, self.rank, self.count, self.box, self.own = axis, rank, count, box, own
        self.send, self.recv = send, recv

    def copy(self, k):
        peer = lax.rem(self.rank + k, self.count)
        own = self.own.at[peer] if len(self.own.shape) == len(self.box.shape) else self.own
        return remote(
            own, self.box.at[self.rank], self.send.at[k], self.recv.at[self.rank], self.axis, peer
        )

    def start(self):
        for k in range(1, self.count):
            self.copy(k).start()

    def wait(self):
        for k in range(1, self.count):
            peer = lax.rem(self.rank + k, self.count)
            slot = self.box.at[peer]
            remote(slot, slot, self.send.at[k], self.recv.at[peer], self.axis, peer).wait_recv()

    def total(self):
        value = self.box[0].astype(f32)
        for k in range(1, self.count):
            value += self.box[k].astype(f32)
        return value

    def drain(self):
        for k in range(1, self.count):
            self.copy(k).wait_send()


def rope(x, cosine, sine):
    return x * cosine + pltpu.roll(x, HEAD_SIZE // 2, 1) * sine


def make_kernel(z, names, scratch):
    R, PW, T, D, O, I, C, Y = z.R, z.PW, z.T, z.D, z.O, z.I, z.C, z.Y
    L, S, QC, KC, NC, NW = z.L, z.S, z.QC, z.KC, z.NC, z.NW
    n_tile = pick(NW, (384, 512, 256, 128))

    def kernel(*refs):
        m = Refs()
        work = jax.tree.unflatten(jax.tree.structure(scratch), refs[len(names) :])
        for name, ref in [*zip(names, refs), *work.items()]:
            setattr(m, name, ref)
        t, d = lax.axis_index("tensor"), lax.axis_index("dp")
        a, b = lax.div(t, I), lax.rem(t, I)
        y, core = lax.div(d, C), lax.rem(d, C)
        place = (a, b)
        lane = lax.broadcasted_iota(jnp.int32, (1, LANES), 1)

        held, normed, W, WO, acc = m.held, m.normed, m.W, m.WO, m.acc

        def to_lanes(column):
            eye = lax.broadcasted_iota(jnp.int32, (R, z.Rp), 0) == lax.broadcasted_iota(
                jnp.int32, (R, z.Rp), 1
            )
            return jnp.sum(jnp.where(eye, column, 0.0), axis=0, keepdims=True)

        def to_column(row):
            eye = lax.broadcasted_iota(jnp.int32, (R, z.Rp), 0) == lax.broadcasted_iota(
                jnp.int32, (R, z.Rp), 1
            )
            return jnp.sum(jnp.where(eye, row, 0.0), axis=1, keepdims=True)

        def stack_rows(rows):
            index = lax.broadcasted_iota(jnp.int32, (8, z.Rp), 0)
            out = jnp.zeros((8, z.Rp), f32)
            for i, row in enumerate(rows):
                out = jnp.where(index == i, row, out)
            return out

        def chunks(fn, total=R):
            @pl.loop(0, total // z.step)
            def _(i):
                fn(pl.ds(pl.multiple_of(i * z.step, 16), z.step))

        emitted = []

        def emit(ref, out):
            copy = pltpu.make_async_copy(ref, out, m.emit[0].at[len(emitted)])
            copy.start()
            emitted.append(copy)

        def exchange(refs, count=T, axis="tensor", rank=t):
            return Exchange(axis, rank, count, *refs)

        loads = [
            (m.pol_hidden, held.at[t, pl.ds(0, R)]),
            (m.ref_hidden, held.at[t, pl.ds(R, R)]),
            (m.w_query, W.at[d, :, pl.ds(0, QC)]),
            (m.w_key, W.at[d, :, pl.ds(QC, KC)]),
            (m.value_projection, W.at[d, :, pl.ds(QC + KC, KC)]),
            (m.a_query, m.a_in.at[0]),
            (m.a_value, m.a_in.at[1]),
            (m.w_out, WO.at[d]),
            (m.query_factor_hbm, m.query_second_factor),
            (m.value_factor_hbm, m.value_second_factor),
            (m.pre_rows, m.gains.at[pl.ds(0, T)]),
            (m.post_rows, m.gains.at[pl.ds(T, T)]),
            (m.readout_hbm, m.readout),
            (m.cosine_hbm, m.cosine),
            (m.sine_hbm, m.sine),
        ]
        copies = [
            pltpu.make_async_copy(src, dst, m.load[0].at[i]) for i, (src, dst) in enumerate(loads)
        ]
        for copy in copies:
            copy.start()

        barrier = pltpu.get_barrier_semaphore()
        for k in range(1, T):
            pl.semaphore_signal(
                barrier, inc=1, device_id={"tensor": lax.rem(t + k, T)}, device_id_type=MESH
            )
        for k in range(1, D):
            pl.semaphore_signal(
                barrier, inc=1, device_id={"dp": lax.rem(d + k, D)}, device_id_type=MESH
            )

        acc[...] = jnp.zeros_like(acc)
        for s in range(S):
            slot = lax.broadcasted_iota(jnp.int32, (L, 1), 0)
            m.liv[s * L : (s + 1) * L, :] = (slot < m.lengths[s]).astype(f32)

        def square(rows):
            x = held[t, rows, :].astype(f32)
            m.col[rows, :] = jnp.sum(x * x, axis=1, keepdims=True)

        stats0 = exchange(m.s0)
        copies[0].wait()
        copies[1].wait()
        chunks(square, 2 * R)
        stats0.own[...] = stack_rows([to_lanes(m.col[0:R]), to_lanes(m.col[R:])])
        stats0.box[t] = stats0.own[...]
        pl.semaphore_wait(barrier, T - 1 + D - 1)
        stats0.start()

        hid = [Gather(z, place, held, m.hid[model], model * R) for model in range(2)]
        hid[0].start()
        hid[1].start()

        def weight_copy(job, slot, piece, k, far):
            buf, (recv, across, beside) = job
            block = buf.at[slot, pl.ds(piece * PW, PW)]
            if far:
                send = across.at[(k - 1) * z.r + piece]
                rank = lax.rem(y + k, Y) * C + core
            else:
                send = beside.at[(lax.div(slot, C) * (C - 1) + k - 1) * z.r + piece]
                rank = y * C + lax.rem(core + k, C)
            return remote(block, block, send, recv.at[slot * z.r + piece], "dp", rank)

        def order_of(q):
            return lax.rem(b + 1 + q, z.r)

        def weights_start(job):
            for q in range(z.r):
                for k in range(1, Y):
                    weight_copy(job, d, order_of(q), k, True).start()
                for k in range(1, C):
                    weight_copy(job, d, order_of(q), k, False).start()

        def weights_wait(job, slot, piece):
            weight_copy(job, slot, piece, 1, Y > 1).wait_recv()

        def weights_relay(job, q):
            for jj in range(1, Y):
                slot = lax.rem(y + jj, Y) * C + core
                weights_wait(job, slot, order_of(q))
                for k in range(1, C):
                    weight_copy(job, slot, order_of(q), k, False).start()

        def weights_wait_core(job, yy, q):
            for k in range(1, C):
                weights_wait(job, yy * C + lax.rem(core + k, C), order_of(q))

        def weights_drain(job):
            for q in range(z.r):
                for k in range(1, Y):
                    weight_copy(job, d, order_of(q), k, True).wait_send()
                for yy in range(Y):
                    for k in range(1, C):
                        weight_copy(job, yy * C + core, order_of(q), k, False).wait_send()

        wq, wo = (W, m.wq), (WO, m.wo)
        for copy in copies[2:7]:
            copy.wait()
        size = pick(z.r * PW, (96, 48, 32, 16))

        @pl.loop(0, z.r * PW // size)
        def _(i):
            at = pl.ds(pl.multiple_of(i * size, 16), size)
            W[d, at, NC:NW] = jnp.concatenate([m.a_in[0, at, :], m.a_in[1, at, :]], axis=1)

        weights_start(wq)
        copies[7].wait()
        weights_start(wo)
        for copy in copies[8:]:
            copy.wait()
        m.F[...] = jnp.zeros_like(m.F)
        m.F[0 : z.rank, 0:QC] = m.query_second_factor[...]
        m.F[z.rank :, QC:] = m.value_second_factor[...]

        stats0.wait()

        scale = lax.rsqrt(stats0.total() / z.W + NORM_EPS)
        m.scol[0:R, :] = to_column(scale[0:1])
        m.scol[R:, :] = to_column(scale[1:2])

        def normalise(model, slot):
            gain = m.gains[pl.ds(slot, 1), :]

            def one(rows):
                at = pl.ds(pl.multiple_of(model * R + rows.start, 16), rows.size)
                x = held[slot, at, :].astype(f32)
                normed[slot, at, :] = (x * m.scol[at, :] * gain).astype(bf16)

            chunks(one)

        def arrive(model, aa):
            hid[model].wait_inner(aa)

            @pl.loop(0, I)
            def _(bb):
                normalise(model, aa * I + bb)

        def project(model, slot):
            row, count = model * R, R
            ws, off = lax.div(slot, z.r), lax.rem(slot, z.r) * PW

            @pl.loop(0, NW // n_tile)
            def _(i):
                cols = pl.ds(pl.multiple_of(i * n_tile, LANES), n_tile)
                acc[row : row + count, cols] += dot(
                    normed[slot, row : row + count, :],
                    W[ws, pl.ds(pl.multiple_of(off, 16), PW), cols],
                )

        def project_group(model, aa, stages):
            @pl.loop(0, I)
            def _(bb):
                slot = aa * I + bb
                near = lax.div(lax.div(slot, z.r), C) == y
                first = lax.rem(slot, z.r) != order_of(z.r - 1)
                kinds = [
                    near,
                    jnp.logical_not(near) & first,
                    jnp.logical_not(near) & jnp.logical_not(first),
                ]
                wanted = kinds[stages[0]]
                for stage in stages[1:]:
                    wanted = wanted | kinds[stage]

                @pl.when(wanted)
                def _():
                    project(model, slot)

        side = jnp.minimum(a, O - 1 - a)

        def visit(j):
            inside = jnp.where(lax.rem(j, 2) == 1, a - lax.div(j + 1, 2), a + lax.div(j, 2))
            outside = jnp.where(a <= O - 1 - a, a + j - side, a - j + side)
            return jnp.where(j <= 2 * side, inside, outside)

        for q in range(z.r):
            weights_wait_core(wq, y, q)

        @pl.loop(1, O)
        def _(j):
            hid[0].relay(visit(j))
            arrive(0, visit(j - 1))
            project_group(0, visit(j - 1), [0])

        for q in range(z.r - 1):
            weights_relay(wq, q)
            for jj in range(1, Y):
                weights_wait_core(wq, lax.rem(y + jj, Y), q)

        hid[1].relay(visit(1))
        arrive(0, visit(O - 1))
        project_group(0, visit(O - 1), [0])

        @pl.loop(0, O)
        def _(j):
            project_group(0, j, [1])

        @pl.loop(2, O)
        def _(j):
            hid[1].relay(visit(j))

        @pl.when(side > 0)
        def _():
            arrive(1, visit(0))
            project_group(1, visit(0), [0, 1])

        weights_relay(wq, z.r - 1)
        for jj in range(1, Y):
            weights_wait_core(wq, lax.rem(y + jj, Y), z.r - 1)

        @pl.loop(0, O)
        def _(j):
            project_group(0, j, [2])

        row_slot = lax.broadcasted_iota(jnp.int32, (L, L), 0)
        key_slot = lax.broadcasted_iota(jnp.int32, (L, L), 1)
        causal = key_slot <= row_slot

        def attend(model):
            base = model * R
            if model == 0:
                m.low[...] = acc[0:R, NC:NW].astype(bf16)
                m.added[...] = ADAPTER_SCALE * dot(m.low[...], m.F[...])

            @pl.loop(0, S)
            def _(s):
                rows = pl.ds(pl.multiple_of(base + s * L, 16), L)
                local = pl.ds(pl.multiple_of(s * L, 16), L)
                allowed = causal & (key_slot < m.lengths[s])
                allowed = jnp.concatenate([allowed.astype(f32)] * z.G, axis=0) > 0.5
                cosine, sine = m.cosine[...], m.sine[...]
                for k in range(z.KV):
                    head = slice(k * HEAD_SIZE, (k + 1) * HEAD_SIZE)
                    kh = acc[rows, QC + k * HEAD_SIZE : QC + (k + 1) * HEAD_SIZE]
                    vh = acc[rows, QC + KC + k * HEAD_SIZE : QC + KC + (k + 1) * HEAD_SIZE]
                    if model == 0:
                        vh = vh + m.added[local, QC + k * HEAD_SIZE : QC + (k + 1) * HEAD_SIZE]
                    kh = rope(kh, cosine, sine).astype(bf16)
                    vh = vh.astype(bf16)
                    queries = []
                    for g in range(z.G):
                        h = k * z.G + g
                        qh = acc[rows, h * HEAD_SIZE : (h + 1) * HEAD_SIZE]
                        if model == 0:
                            qh = qh + m.added[local, h * HEAD_SIZE : (h + 1) * HEAD_SIZE]
                        queries.append(rope(qh, cosine, sine).astype(bf16))
                    q2 = jnp.concatenate(queries, axis=0)
                    scores = dot(q2, kh, NT) * query_scale()
                    capped = SOFT_CAP * jnp.tanh(scores / SOFT_CAP)
                    weights = jnp.where(allowed, jnp.exp(capped), 0.0)
                    probs = weights / jnp.sum(weights, axis=1, keepdims=True)
                    out = dot(probs.astype(bf16), vh).astype(bf16)
                    for g in range(z.G):
                        h = k * z.G + g
                        m.mixed[rows, h * HEAD_SIZE : (h + 1) * HEAD_SIZE] = out[
                            g * L : (g + 1) * L
                        ]
                    if model == 0:
                        m.q2[s, k] = q2
                        m.kk[s, k] = kh
                        m.vv[s, k] = vh
                        m.probs[s, k] = probs
                        m.capped[s, k] = capped

        attend(0)

        def out_term(model):
            def term(slot):
                ws, off = lax.div(slot, z.r), lax.rem(slot, z.r) * PW
                return dot(
                    m.mixed[model * R : (model + 1) * R, :],
                    WO[ws, pl.ds(pl.multiple_of(off, 16), PW), :],
                    NT,
                )

            return term

        def reduce_of(bufs, sems, out, row):
            return Reduce(
                z,
                place,
                bufs,
                sems,
                m.piece,
                out,
                row,
            )

        red_pol = reduce_of(m.pol, m.pol_sems, m.summed, 0)
        red_ref = reduce_of(m.ref, m.ref_sems, m.summed, R)
        red_grad = reduce_of(m.pol, m.grad_sems, m.gnorm, 0)

        def near_first(j):
            yy, jj = lax.rem(y + lax.div(j, z.gp), Y), lax.rem(j, z.gp)
            low = yy * z.gp + jj
            high = yy * z.gp + z.gp - 1 - jj
            return jnp.where(2 * yy < Y, low, high)

        def far_first(j):
            return visit(O - 1 - j)

        def produce_range(red, first, last, order, term, ks):
            @pl.loop(first, last)
            def _(j):
                for k in ks:
                    red.produce(order(j), k, term)

        def collect_stage(red, j, order, distance=None):
            aa = order(j)
            ahead = jnp.where(aa > a, a, O - 1 - a)
            wanted = aa != a if distance is None else (aa != a) & (ahead == distance)

            @pl.when(wanted)
            def _():
                red.collect(aa)

        def collect_range(red, first, last, order, distance=None):
            @pl.loop(first, last)
            def _(j):
                collect_stage(red, j, order, distance)

        xs, own = list(range(1, I)), [0]
        for q in range(z.r):
            weights_wait_core(wo, y, q)
        produce_range(red_pol, 0, z.gp, near_first, out_term(0), xs + own)
        early = z.r if I != z.r else z.r - 1
        for q in range(early):
            weights_relay(wo, q)
            for jj in range(1, Y):
                weights_wait_core(wo, lax.rem(y + jj, Y), q)
        produce_range(red_pol, z.gp, O, near_first, out_term(0), xs)

        @pl.loop(0, O)
        def _(j):
            @pl.when((j > 0) | (side == 0))
            def _():
                arrive(1, visit(j))
                project_group(1, visit(j), [0, 1])

            @pl.when(j == 1)
            def _():
                collect_range(red_pol, 0, 1, near_first, 0)

        collect_range(red_pol, 1, z.gp, near_first, 0)
        for q in range(early, z.r):
            weights_relay(wo, q)

        for q in range(early, z.r):
            for jj in range(1, Y):
                weights_wait_core(wo, lax.rem(y + jj, Y), q)
        produce_range(red_pol, z.gp, O, near_first, out_term(0), own)
        collect_range(red_pol, 0, z.gp, near_first, 1)
        collect_range(red_pol, z.gp, z.gp + 1, near_first, 0)

        @pl.loop(0, O)
        def _(j):
            project_group(1, j, [2])

        attend(1)
        produce_range(red_ref, 0, 2, far_first, out_term(1), xs + own)

        for distance in range(2, O - 1):
            collect_range(red_pol, 0, z.gp, near_first, distance)

        @pl.loop(1, O - 1 + 2 * (O - 1 - z.gp))
        def _(turn):
            @pl.loop(z.gp, O)
            def _(j):
                collect_stage(red_pol, j, near_first, turn - 2 * (j - z.gp))

        produce_range(red_ref, 2, O - 1, far_first, out_term(1), xs + own)
        red_pol.collect(a)

        post_gain = m.gains[pl.ds(T + t, 1), :]

        def token_sums(model, refs):
            base = model * R

            def one(rows):
                at = pl.ds(base + rows.start, rows.size)
                x = m.summed[at, :]
                read = m.readout[rows, :].astype(f32)
                m.pcol[pl.ds(rows.start, rows.size), :] = jnp.sum(x * x, axis=1, keepdims=True)
                m.pcol[pl.ds(R + rows.start, rows.size), :] = jnp.sum(
                    x * (post_gain * read), axis=1, keepdims=True
                )
                h = held[t, at, :].astype(f32)
                m.pcol[pl.ds(2 * R + rows.start, rows.size), :] = jnp.sum(
                    h * read, axis=1, keepdims=True
                )

            chunks(one)
            done = exchange(refs)
            done.own[...] = stack_rows([to_lanes(m.pcol[i * R : (i + 1) * R]) for i in range(3)])
            done.box[t] = done.own[...]
            done.start()
            return done

        stats1 = token_sums(0, m.s1)
        collect_range(red_ref, 0, 2, far_first, 0)
        stats1.wait()
        sums1 = stats1.total()
        post1 = lax.rsqrt(sums1[0:1] / z.W + NORM_EPS)
        m.col[0:R, :] = to_column(post1)
        m.col[R:, :] = to_column(post1 * post1 * post1 * sums1[1:2] / z.W)

        def make_grad(rows):
            read = m.readout[rows, :].astype(f32)
            value = m.col[rows, :] * post_gain * read - m.summed[rows, :] * m.col[
                pl.ds(R + rows.start, rows.size), :
            ]
            m.gheld[t, rows, :] = (value * m.liv[rows, :]).astype(bf16)

        chunks(make_grad)
        gag = Gather(z, place, m.gheld, m.gag)
        gag.start()

        def finish(model, out):
            def one(rows):
                at = pl.ds(model * R + rows.start, rows.size)
                h = held[t, at, :].astype(f32)
                out[rows, :] = (h + m.summed[at, :] * m.pcol[rows, :] * post_gain).astype(
                    bf16
                )

            chunks(one)

        m.pcol[0:R, :] = m.col[0:R, :]
        finish(0, m.policy_out)
        emit(m.policy_out, m.out_policy)
        m.gm[...] = jnp.zeros_like(m.gm)

        def back_out(aa):
            @pl.loop(0, I)
            def _(bb):
                slot = aa * I + bb
                ws, off = lax.div(slot, z.r), lax.rem(slot, z.r) * PW
                m.gm[...] += dot(
                    m.gheld[slot], WO[ws, pl.ds(pl.multiple_of(off, 16), PW), :]
                )

        collect_range(red_ref, 2, O - 1, far_first, 0)

        @pl.loop(1, O)
        def _(j):
            gag.relay(visit(j))
            gag.wait_inner(visit(j - 1))
            back_out(visit(j - 1))

        produce_range(red_ref, O - 1, O, far_first, out_term(1), xs + own)
        collect_range(red_ref, 0, O - 1, far_first, 1)
        gag.wait_inner(visit(O - 1))
        back_out(visit(O - 1))
        for distance in range(2, O - 1):
            collect_range(red_ref, 0, O - 1, far_first, distance)
        m.gmb[...] = m.gm[...].astype(bf16)

        @pl.loop(0, S)
        def _(s):
            rows = pl.ds(pl.multiple_of(s * L, 16), L)
            cosine, sine = m.cosine[...], -m.sine[...]
            for k in range(z.KV):
                parts = []
                for g in range(z.G):
                    h = k * z.G + g
                    parts.append(m.gmb[rows, h * HEAD_SIZE : (h + 1) * HEAD_SIZE])
                grad = jnp.concatenate(parts, axis=0)
                probs, capped = m.probs[s, k], m.capped[s, k]
                grad_probs = dot(grad, m.vv[s, k], NT)
                grad_v = dot(probs.astype(bf16), grad, TN)
                centered = grad_probs - jnp.sum(grad_probs * probs, axis=1, keepdims=True)
                ratio = capped / SOFT_CAP
                grad_scores = (
                    probs * centered * (1.0 - ratio * ratio) * query_scale()
                ).astype(bf16)
                grad_q = dot(grad_scores, m.kk[s, k])
                grad_k = dot(grad_scores, m.q2[s, k], TN)
                for g in range(z.G):
                    h = k * z.G + g
                    m.dcat[rows, h * HEAD_SIZE : (h + 1) * HEAD_SIZE] = rope(
                        grad_q[g * L : (g + 1) * L], cosine, sine
                    ).astype(bf16)
                at = QC + k * HEAD_SIZE
                m.dcat[rows, at : at + HEAD_SIZE] = rope(grad_k, cosine, sine).astype(bf16)
                m.dcat[rows, at + KC : at + KC + HEAD_SIZE] = grad_v.astype(bf16)

        m.dcat[:, NC:NW] = (
            ADAPTER_SCALE
            * (
                dot(m.dcat[:, 0:QC], m.F[:, 0:QC], NT)
                + dot(m.dcat[:, QC + KC : NC], m.F[:, QC:], NT)
            )
        ).astype(bf16)

        def in_term(slot):
            ws, off = lax.div(slot, z.r), lax.rem(slot, z.r) * PW
            return dot(m.dcat[...], W[ws, pl.ds(pl.multiple_of(off, 16), PW), :], NT)

        def pre_dot(rows):
            m.pcol[pl.ds(3 * R + rows.start, rows.size), :] = jnp.sum(
                m.dcat[rows, :].astype(f32) * acc[rows, :], axis=1, keepdims=True
            )

        def hook_part(part, k):
            return remote(
                m.dcat.at[pl.ds(pl.multiple_of(part * z.HR, 16), z.HR), pl.ds(NC, z.AR)],
                m.hbox.at[t],
                m.h1[0].at[k],
                m.h1[1].at[t],
                "tensor",
                lax.rem(t + k, T),
            )

        def hook_whole(k):
            mine = m.hsum.at[t]
            peer = lax.rem(t + k, T)
            return remote(mine, mine, m.h2[0].at[k], m.h2[1].at[t], "tensor", peer)

        for k in range(1, T):
            peer = lax.rem(t + k, T)

            @pl.when(peer < z.HN)
            def _(peer=peer, k=k):
                hook_part(peer, k).start()

        chunks(pre_dot)
        stats3 = exchange(m.s3)
        stats3.own[...] = stack_rows([to_lanes(m.pcol[3 * R :])])
        stats3.box[t] = stats3.own[...]
        stats3.start()
        red_pol.drain()
        produce_range(red_grad, 0, 1, far_first, in_term, xs + own)
        red_ref.collect(a)
        stats2 = token_sums(1, m.s2)
        produce_range(red_grad, 1, 2, far_first, in_term, xs + own)

        @pl.when(t < z.HN)
        def _():
            at = pl.ds(pl.multiple_of(t * z.HR, 16), z.HR)
            m.hbox[t] = m.dcat[at, NC:NW]
            for k in range(1, T):
                peer = lax.rem(t + k, T)
                slot = m.hbox.at[peer]
                remote(slot, slot, m.h1[0].at[k], m.h1[1].at[peer], "tensor", peer).wait_recv()
            value = m.hbox[0].astype(f32)
            for k in range(1, T):
                value += m.hbox[k].astype(f32)
            m.hsum[t] = value.astype(bf16)
            for k in range(1, T):
                hook_whole(k).start()

        produce_range(red_grad, 2, O, far_first, in_term, xs + own)
        collect_range(red_grad, 0, 1, far_first)
        stats2.wait()
        sums2 = stats2.total()
        post2 = lax.rsqrt(sums2[0:1] / z.W + NORM_EPS)

        token_pol = sums1[2:3] + post1 * sums1[1:2]
        token_ref = sums2[2:3] + post2 * sums2[1:2]
        wide = lax.broadcasted_iota(jnp.int32, (1, z.Rp), 1)
        mine = jnp.zeros((1, LANES), f32)
        for s in range(S):
            inside = (wide >= s * L) & (wide < s * L + m.lengths[s])
            value = jnp.sum(jnp.where(inside, token_pol, 0.0), axis=1, keepdims=True) - jnp.sum(
                jnp.where(inside, token_ref, 0.0), axis=1, keepdims=True
            )
            mine = jnp.where(lane == d * S + s, value, mine)
        scores = exchange(m.score, D, "dp", d)
        scores.own[...] = jnp.broadcast_to(mine, (8, LANES))
        scores.box[d] = scores.own[...]
        scores.start()
        collect_range(red_grad, 1, 2, far_first)
        scores.wait()
        ratios = scores.total()[0:1]
        loss = jnp.zeros((1, 1), f32)
        coefficients = jnp.zeros((1, LANES), f32)
        for k in range(S * D // 2):
            chosen, rejected = m.pairing[2 * k], m.pairing[2 * k + 1]
            margin = DPO_BETA * (
                jnp.sum(jnp.where(lane == chosen, ratios, 0.0), axis=1, keepdims=True)
                - jnp.sum(jnp.where(lane == rejected, ratios, 0.0), axis=1, keepdims=True)
            )
            soft = jnp.exp(-jnp.abs(margin))
            loss += jnp.maximum(-margin, 0.0) + jnp.log1p(soft)
            sigmoid = jnp.where(margin > 0, soft, 1.0) / (1.0 + soft)
            pull = DPO_BETA * LOSS_SCALE * sigmoid
            coefficients += jnp.where(lane == rejected, pull, 0.0) - jnp.where(
                lane == chosen, pull, 0.0
            )
        m.dpo_loss[...] = jnp.broadcast_to(loss, (8, LANES))
        emit(m.dpo_loss, m.out_loss)
        own_coef = []
        for s in range(S):
            value = jnp.sum(jnp.where(lane == d * S + s, coefficients, 0.0), axis=1, keepdims=True)
            own_coef.append(value)
            m.ccol[s * L : (s + 1) * L, :] = jnp.broadcast_to(value, (L, 1))

        parts_q = jnp.zeros((z.rank, QC), f32)
        parts_v = jnp.zeros((z.rank, KC), f32)
        for s in range(S):
            rows = slice(s * L, (s + 1) * L)
            low = m.low[rows, :]
            parts_q += own_coef[s] * dot(low, m.dcat[rows, 0:QC], TN)[0 : z.rank]
            parts_v += own_coef[s] * dot(low, m.dcat[rows, QC + KC : NC], TN)[z.rank :]
        factors = exchange(m.fac, D, "dp", d)
        factors.own[:, 0:QC] = (ADAPTER_SCALE * parts_q).astype(bf16)
        factors.own[:, QC:] = (ADAPTER_SCALE * parts_v).astype(bf16)
        factors.box[d] = factors.own[...]
        factors.start()

        for k in range(1, T):
            peer = lax.rem(t + k, T)

            @pl.when(peer < z.HN)
            def _(peer=peer, k=k):
                slot = m.hsum.at[peer]
                remote(slot, slot, m.h2[0].at[k], m.h2[1].at[peer], "tensor", peer).wait_recv()

        hook = m.hsum[...].reshape(R, z.AR)
        hook = (hook.astype(f32) * m.ccol[...]).astype(bf16)
        adapters = exchange(m.ad, D, "dp", d)

        @pl.loop(0, T)
        def _(slot):
            ws, off = lax.div(slot, z.r), lax.rem(slot, z.r) * PW
            adapters.own[ws, pl.ds(pl.multiple_of(off, 16), PW), :] = dot(
                normed[slot, 0:R, :], hook, TN
            ).astype(bf16)

        adapters.box[d] = adapters.own[d]
        adapters.start()
        collect_range(red_grad, 2, O - 1, far_first)
        m.pcol[0:R, :] = to_column(post2)
        finish(1, m.reference_out)
        emit(m.reference_out, m.out_reference)
        stats3.wait()
        m.pcol[0:R, :] = to_column(stats3.total()[0:1])
        factors.wait()
        value = factors.total()
        m.query_factor_gradient[...] = value[:, 0:QC]
        m.value_factor_gradient[...] = value[:, QC:]
        emit(m.query_factor_gradient, m.out_query)
        emit(m.value_factor_gradient, m.out_value)
        red_grad.collect(a)

        pre_gain = m.gains[pl.ds(t, 1), :]

        def grad_in(rows):
            read = m.readout[rows, :].astype(f32) * m.liv[rows, :]
            scale = m.scol[rows, :]
            h = held[t, rows, :].astype(f32)
            value = (
                read
                + scale * pre_gain * m.gnorm[rows, :]
                - h * (scale * scale * m.pcol[rows, :] / z.W)
            )
            m.grad_hidden[rows, :] = (value * m.ccol[rows, :]).astype(bf16)

        chunks(grad_in)
        emit(m.grad_hidden, m.out_hidden)
        adapters.wait()

        def sum_adapters(rows):
            value = adapters.box[0, rows, :].astype(f32)
            for k in range(1, D):
                value += adapters.box[k, rows, :].astype(f32)
            m.grad_a[rows, :] = value

        @pl.loop(0, z.r * PW // size)
        def _(i):
            sum_adapters(pl.ds(pl.multiple_of(i * size, 16), size))

        emit(m.grad_a, m.out_adapter)

        hid[0].drain()
        hid[1].drain()
        gag.drain()
        red_ref.drain()
        red_grad.drain()
        weights_drain(wq)
        weights_drain(wo)
        for done in (stats0, stats1, stats2, stats3, scores, factors, adapters):
            done.drain()
        for k in range(1, T):
            peer = lax.rem(t + k, T)

            @pl.when(peer < z.HN)
            def _(peer=peer, k=k):
                hook_part(peer, k).wait_send()

        @pl.when(t < z.HN)
        def _():
            for k in range(1, T):
                hook_whole(k).wait_send()

        for copy in emitted:
            copy.wait()

    return kernel


def hand_over(arrays):
    count = len(arrays)
    shapes = [array.shape if array.shape != (8, LANES) else (1, 1) for array in arrays]

    def kernel(*refs):
        ins, outs, held = refs[:count], refs[count : 2 * count], refs[2 * count : 3 * count]
        came, left = refs[3 * count :]
        arrivals = [
            pltpu.make_async_copy(src, dst, came.at[i])
            for i, (src, dst) in enumerate(zip(ins, held))
        ]
        for copy in arrivals:
            copy.start()
        exits = []
        for i, copy in enumerate(arrivals):
            copy.wait()
            if shapes[i] == (1, 1):
                outs[i][...] = held[i][0:1, 0:1]
            else:
                exits.append(pltpu.make_async_copy(held[i], outs[i], left.at[i]))
                exits[-1].start()
        for copy in exits:
            copy.wait()

    hbm = pl.BlockSpec(memory_space=pl.ANY)
    return pl.pallas_call(
        kernel,
        name="hand_over",
        out_shape=[jax.ShapeDtypeStruct(s, a.dtype) for s, a in zip(shapes, arrays)],
        in_specs=[hbm] * count,
        out_specs=[pl.BlockSpec(memory_space=pltpu.VMEM) if s == (1, 1) else hbm for s in shapes],
        scratch_shapes=[pltpu.VMEM(a.shape, a.dtype) for a in arrays]
        + [pltpu.SemaphoreType.DMA((count,)), pltpu.SemaphoreType.DMA((count,))],
    )(*arrays)


def body(
    ref_hidden,
    pol_hidden,
    readout,
    lengths,
    pairing,
    pre_gain,
    post_gain,
    w_query,
    w_key,
    value_projection,
    w_out,
    a_query,
    a_value,
    query_second_factor,
    value_second_factor,
):
    z = Sizes(
        pol_hidden.shape[0],
        pol_hidden.shape[1],
        lengths.shape[0],
        lax.axis_size("dp"),
        lax.axis_size("tensor"),
        w_query.shape[1],
        w_key.shape[1],
        query_second_factor.shape[0],
    )
    cosine, sine = rope_tables(z.L)
    smem = pl.BlockSpec(memory_space=pltpu.SMEM)
    hbm = pl.BlockSpec(memory_space=pl.ANY)
    inputs = dict(
        pol_hidden=pol_hidden,
        ref_hidden=ref_hidden,
        readout_hbm=readout,
        lengths=lengths,
        pairing=pairing,
        pre_rows=pre_gain.reshape(z.T, z.PW),
        post_rows=post_gain.reshape(z.T, z.PW),
        w_query=w_query,
        w_key=w_key,
        value_projection=value_projection,
        w_out=w_out,
        a_query=a_query,
        a_value=a_value,
        query_factor_hbm=query_second_factor,
        value_factor_hbm=value_second_factor,
        cosine_hbm=jnp.asarray(cosine),
        sine_hbm=jnp.asarray(sine),
    )
    outputs = dict(
        out_policy=((z.R, z.PW), bf16),
        out_reference=((z.R, z.PW), bf16),
        out_loss=((8, LANES), f32),
        out_hidden=((z.R, z.PW), bf16),
        out_adapter=((z.r * z.PW, z.AR), f32),
        out_query=((z.rank, z.QC), f32),
        out_value=((z.rank, z.KC), f32),
    )
    scratch = build_scratch(z)
    outs = pl.pallas_call(
        make_kernel(z, [*inputs, *outputs], scratch),
        name="preference_step",
        out_shape=[jax.ShapeDtypeStruct(*entry) for entry in outputs.values()],
        in_specs=[smem if array.ndim == 1 else hbm for array in inputs.values()],
        out_specs=[hbm] * len(outputs),
        scratch_shapes=jax.tree.leaves(scratch),
        compiler_params=pltpu.CompilerParams(
            collective_id=1, has_side_effects=True, vmem_limit_bytes=VMEM_GRANT
        ),
    )(*inputs.values())
    policy_out, reference_out, loss, grad_hidden, grad_a, grad_q, grad_v = hand_over(outs)
    return policy_out, reference_out, loss[0, 0], grad_hidden, grad_a, grad_q, grad_v


def solution(mesh):
    placed = (
        P("dp", "tensor"),
        P("dp", "tensor"),
        P("dp", "tensor"),
        P("dp"),
        P(),
        P(),
        P(),
        P("dp", "tensor"),
        P("dp", "tensor"),
        P("dp", "tensor"),
        P("dp", "tensor"),
        P("dp", None),
        P("dp", None),
        P(None, "tensor"),
        P(None, "tensor"),
    )
    return jax.shard_map(
        body,
        mesh=mesh,
        in_specs=placed,
        out_specs=(
            P("dp", "tensor"),
            P("dp", "tensor"),
            P(),
            P("dp", "tensor"),
            P("dp", None),
            P(None, "tensor"),
            P(None, "tensor"),
        ),
        check_vma=False,
    )
```

```python
import jax
import jax.numpy as jnp
import numpy as np
from jax import lax
from jax.experimental import pallas as pl
from jax.experimental.pallas import tpu as pltpu
from jax.sharding import PartitionSpec as P

MODEL_WIDTH = 4608
HQ = 32
HEAD_SIZE = 128


NORM_EPS = 1e-06
SOFT_CAP = 50.0
ADAPTER_SCALE = 0.5
DPO_BETA = 0.5
LOSS_SCALE = 256.0
ROPE_BASE = 10000.0

MESH = pl.DeviceIdType.MESH
VMEM_GRANT = 67_000_000
LANES = 128
f32, bf16 = jnp.float32, jnp.bfloat16
NT = (((1,), (1,)), ((), ()))
TN = (((0,), (0,)), ((), ()))


def query_scale():
    return float(MODEL_WIDTH // HQ) ** (-0.5)


def grid_of(axis, count):
    if axis == "dp":
        inner = 2 if count % 2 == 0 else 1
    else:
        inner = 1
        while (inner * 2) ** 2 <= count and count % (inner * 2) == 0:
            inner *= 2
    return count // inner, inner


def pick(size, options):
    for option in options:
        if size % option == 0:
            return option
    return size


def rope_tables(length):
    half = HEAD_SIZE // 2
    spacing = ROPE_BASE ** (-2.0 * np.arange(half, dtype=np.float32) / HEAD_SIZE)
    angles = np.arange(length, dtype=np.float32)[:, None] * spacing[None, :].astype(np.float32)
    cosine, sine = np.cos(angles), np.sin(angles)
    return (
        np.concatenate([cosine, cosine], axis=1).astype(np.float32),
        np.concatenate([-sine, sine], axis=1).astype(np.float32),
    )


def dot(x, y, dims=(((1,), (0,)), ((), ()))):
    return lax.dot_general(x, y, dims, preferred_element_type=f32)


def remote(src, dst, send_sem, recv_sem, axis, rank):
    return pltpu.make_async_remote_copy(
        src_ref=src,
        dst_ref=dst,
        send_sem=send_sem,
        recv_sem=recv_sem,
        device_id={axis: rank},
        device_id_type=MESH,
    )


class Sizes:
    def __init__(self, tok_rows, part_width, seqs, dp, tensor, q_cols, k_cols, rank):
        self.R, self.PW, self.S, self.D, self.T = tok_rows, part_width, seqs, dp, tensor
        self.L = tok_rows // seqs
        self.QC, self.KC = q_cols, k_cols
        self.AR = 2 * rank
        self.rank = rank
        self.NC = q_cols + 2 * k_cols
        self.NW = self.NC + self.AR
        self.O, self.I = grid_of("tensor", tensor)
        self.Y, self.C = grid_of("dp", dp)
        self.r = tensor // dp
        self.gp = max(self.O // self.Y, 1)
        self.KV = k_cols // HEAD_SIZE
        self.G = q_cols // k_cols
        self.P = self.L
        self.n = tok_rows // self.P
        self.Rp = -(-tok_rows // LANES) * LANES
        self.W = part_width * tensor
        self.step = pick(tok_rows, (48, 32, 16))
        size = 16
        while tok_rows % size or tok_rows // size > tensor:
            size += 16
        self.HR, self.HN = size, tok_rows // size


def vm(*shape, kind=bf16):
    return pltpu.VMEM(shape, kind)


def sem(*counts):
    return [pltpu.SemaphoreType.DMA((max(count, 1),)) for count in counts]


def build_scratch(z):
    R, PW, T, D, O, I, n = z.R, z.PW, z.T, z.D, z.O, z.I, z.n
    inner = O * (I - 1)
    moved = z.QC + z.KC

    def boxes():
        return [vm(T, R, PW), vm(max(inner, 1), R, PW), vm(O, R, PW), vm(O, R, PW)]

    def reduce_sems():
        return sem(inner * n, inner * n, O * n, O * n, O * n)

    def gather_sems(count):
        return sem(T * count, O * count, O * count, inner * count)

    def stat():
        return [vm(T, 8, z.Rp, kind=f32), vm(8, z.Rp, kind=f32)] + sem(T, T)

    def weight_sems():
        return sem(D * z.r, (z.Y - 1) * z.r, z.Y * (z.C - 1) * z.r)

    return dict(
        held=vm(T, 2 * R, PW),
        normed=vm(T, 2 * R, PW),
        W=vm(D, z.r * PW, z.NW),
        WO=vm(D, z.r * PW, z.QC),
        acc=vm(2 * R, z.NW, kind=f32),
        added=vm(R, moved, kind=f32),
        low=vm(R, z.AR),
        F=vm(z.AR, moved),
        q2=vm(z.S, z.KV, z.G * z.L, HEAD_SIZE),
        kk=vm(z.S, z.KV, z.L, HEAD_SIZE),
        vv=vm(z.S, z.KV, z.L, HEAD_SIZE),
        probs=vm(z.S, z.KV, z.G * z.L, z.L, kind=f32),
        capped=vm(z.S, z.KV, z.G * z.L, z.L, kind=f32),
        mixed=vm(2 * R, z.QC),
        pol=boxes(),
        ref=boxes(),
        pol_sems=reduce_sems(),
        ref_sems=reduce_sems(),
        grad_sems=reduce_sems(),
        piece=vm(z.P, PW, kind=f32),
        summed=vm(2 * R, PW, kind=f32),
        gheld=vm(T, R, PW),
        gm=vm(R, z.QC, kind=f32),
        gmb=vm(R, z.QC),
        dcat=vm(R, z.NW),
        gnorm=vm(R, PW, kind=f32),
        col=vm(2 * R, 1, kind=f32),
        scol=vm(2 * R, 1, kind=f32),
        liv=vm(R, 1, kind=f32),
        ccol=vm(R, 1, kind=f32),
        pcol=vm(4 * R, 1, kind=f32),
        s0=stat(),
        s1=stat(),
        s2=stat(),
        s3=stat(),
        score=[vm(D, 8, LANES, kind=f32), vm(8, LANES, kind=f32)] + sem(D, D),
        hbox=vm(T, z.HR, z.AR),
        hsum=vm(z.HN, z.HR, z.AR),
        h1=sem(T, T),
        h2=sem(T, T),
        fac=[vm(D, z.rank, moved), vm(z.rank, moved)] + sem(D, D),
        ad=[vm(D, z.r * PW, z.AR), vm(D, z.r * PW, z.AR)] + sem(D, D),
        load=sem(16),
        emit=sem(8),
        a_in=vm(z.AR, z.r * PW),
        query_second_factor=vm(z.rank, z.QC),
        value_second_factor=vm(z.rank, z.KC),
        gains=vm(2 * T, PW, kind=f32),
        readout=vm(R, PW),
        cosine=vm(z.L, HEAD_SIZE, kind=f32),
        sine=vm(z.L, HEAD_SIZE, kind=f32),
        policy_out=vm(R, PW),
        reference_out=vm(R, PW),
        dpo_loss=vm(8, LANES, kind=f32),
        grad_hidden=vm(R, PW),
        grad_a=vm(z.r * PW, z.AR, kind=f32),
        query_factor_gradient=vm(z.rank, z.QC, kind=f32),
        value_factor_gradient=vm(z.rank, z.KC, kind=f32),
        hid=[gather_sems(n), gather_sems(n)],
        gag=gather_sems(n),
        wq=weight_sems(),
        wo=weight_sems(),
    )


class Refs:
    pass


class Gather:
    def __init__(self, z, place, held, sems, row=0):
        self.z, self.place, self.held, self.pieces = z, place, held, z.n
        self.r, self.u, self.d, self.x = sems
        self.row = row

    def block(self, slot, c):
        return self.held.at[slot, pl.ds(self.row + c * self.z.P, self.z.P)]

    def copy(self, aa, c, kind, k=0):
        z, (a, b) = self.z, self.place
        slot = aa * z.I + b
        block = self.block(slot, c)
        at = aa * self.pieces + c
        if kind == "up":
            send, rank = self.u.at[at], lax.rem(a + 1, z.O) * z.I + b
        elif kind == "dn":
            send, rank = self.d.at[at], lax.rem(a + z.O - 1, z.O) * z.I + b
        else:
            send = self.x.at[(aa * (z.I - 1) + k - 1) * self.pieces + c]
            rank = a * z.I + lax.rem(b + k, z.I)
        return remote(block, block, send, self.r.at[slot * self.pieces + c], "tensor", rank)

    def wait_recv(self, slot, c):
        z = self.z
        block = self.block(slot, c)
        at = slot * self.pieces + c
        remote(block, block, self.u.at[0], self.r.at[at], "tensor", 0).wait_recv()

    def sends(self, aa, c, act):
        z, (a, b) = self.z, self.place

        @pl.when((aa <= a) & (a < z.O - 1))
        def _():
            act(self.copy(aa, c, "up"))

        @pl.when((aa >= a) & (a > 0))
        def _():
            act(self.copy(aa, c, "dn"))

        for k in range(1, z.I):
            act(self.copy(aa, c, "x", k))

    def start(self):
        for c in range(self.pieces):
            self.sends(self.place[0], c, lambda copy: copy.start())

    def relay(self, aa):
        z, (a, b) = self.z, self.place

        @pl.loop(0, self.pieces)
        def _(c):
            self.wait_recv(aa * z.I + b, c)
            self.sends(aa, c, lambda copy: copy.start())

    def wait_inner(self, aa):
        z, (a, b) = self.z, self.place
        for k in range(1, z.I):

            @pl.loop(0, self.pieces)
            def _(c, k=k):
                self.wait_recv(aa * z.I + lax.rem(b + k, z.I), c)

    def drain(self):
        @pl.loop(0, self.z.O)
        def _(aa):
            @pl.loop(0, self.pieces)
            def _(c):
                self.sends(aa, c, lambda copy: copy.wait_send())


class Reduce:
    def __init__(self, z, place, bufs, sems, piece, out, out_row):
        self.z, self.place, self.piece = z, place, piece
        self.stage, self.near, self.up, self.dn = bufs
        self.sx, self.rx, self.sz, self.ru, self.rd = sems
        self.out, self.out_row = out, out_row

    def rows(self, c):
        return pl.ds(c * self.z.P, self.z.P)

    def x_copy(self, aa, k, c):
        z, (a, b) = self.z, self.place
        at = aa * (z.I - 1) + k - 1
        return remote(
            self.stage.at[aa * z.I + lax.rem(b + k, z.I), self.rows(c)],
            self.near.at[at, self.rows(c)],
            self.sx.at[at * z.n + c],
            self.rx.at[at * z.n + c],
            "tensor",
            a * z.I + lax.rem(b + k, z.I),
        )

    def z_copy(self, aa, c, up):
        z, (a, b) = self.z, self.place
        box, sem = (self.up, self.ru) if up else (self.dn, self.rd)
        rank = lax.rem(a + (1 if up else z.O - 1), z.O) * z.I + b
        at = aa * z.n + c
        return remote(
            self.stage.at[aa * z.I + b, self.rows(c)],
            box.at[aa, self.rows(c)],
            self.sz.at[at],
            sem.at[at],
            "tensor",
            rank,
        )

    def produce(self, aa, k, term):
        z, (a, b) = self.z, self.place
        slot = aa * z.I + lax.rem(b + k, z.I)
        self.stage[slot] = term(slot).astype(bf16)
        if k:
            for c in range(z.n):
                self.x_copy(aa, k, c).start()

    def collect(self, aa):
        z, (a, b) = self.z, self.place

        @pl.loop(0, z.n)
        def _(c):
            rows = pl.ds(pl.multiple_of(c * z.P, 16), z.P)
            value = self.stage[aa * z.I + b, rows, :].astype(f32)
            for k in range(1, z.I):
                self.x_copy(aa, k, c).wait_recv()
                value += self.near[aa * (z.I - 1) + k - 1, rows, :].astype(f32)
            self.piece[...] = value

            @pl.when((aa >= a) & (a > 0))
            def _():
                self.z_copy(aa, c, True).wait_recv()
                self.piece[...] += self.up[aa, rows, :].astype(f32)

            @pl.when((aa <= a) & (a < z.O - 1))
            def _():
                self.z_copy(aa, c, False).wait_recv()
                self.piece[...] += self.dn[aa, rows, :].astype(f32)

            @pl.when(aa == a)
            def _():
                at = pl.ds(pl.multiple_of(self.out_row + c * z.P, 8), z.P)
                self.out[at, :] = self.piece[...]

            @pl.when(aa != a)
            def _():
                self.stage[aa * z.I + b, rows, :] = self.piece[...].astype(bf16)

            @pl.when(aa > a)
            def _():
                self.z_copy(aa, c, True).start()

            @pl.when(aa < a)
            def _():
                self.z_copy(aa, c, False).start()

    def drain(self):
        z, (a, b) = self.z, self.place

        @pl.loop(0, z.O)
        def _(aa):
            @pl.loop(0, z.n)
            def _(c):
                for k in range(1, z.I):
                    self.x_copy(aa, k, c).wait_send()

                @pl.when(aa != a)
                def _():
                    self.z_copy(aa, c, True).wait_send()


class Exchange:
    def __init__(self, axis, rank, count, box, own, send, recv):
        self.axis, self.rank, self.count, self.box, self.own = axis, rank, count, box, own
        self.send, self.recv = send, recv

    def copy(self, k):
        peer = lax.rem(self.rank + k, self.count)
        own = self.own.at[peer] if len(self.own.shape) == len(self.box.shape) else self.own
        return remote(
            own, self.box.at[self.rank], self.send.at[k], self.recv.at[self.rank], self.axis, peer
        )

    def start(self):
        for k in range(1, self.count):
            self.copy(k).start()

    def wait(self):
        for k in range(1, self.count):
            peer = lax.rem(self.rank + k, self.count)
            slot = self.box.at[peer]
            remote(slot, slot, self.send.at[k], self.recv.at[peer], self.axis, peer).wait_recv()

    def total(self):
        value = self.box[0].astype(f32)
        for k in range(1, self.count):
            value += self.box[k].astype(f32)
        return value

    def drain(self):
        for k in range(1, self.count):
            self.copy(k).wait_send()


def rope(x, cosine, sine):
    return x * cosine + pltpu.roll(x, HEAD_SIZE // 2, 1) * sine


def make_kernel(z, names, scratch):
    R, PW, T, D, O, I, C, Y = z.R, z.PW, z.T, z.D, z.O, z.I, z.C, z.Y
    L, S, QC, KC, NC, NW = z.L, z.S, z.QC, z.KC, z.NC, z.NW
    n_tile = pick(NW, (384, 512, 256, 128))

    def kernel(*refs):
        m = Refs()
        work = jax.tree.unflatten(jax.tree.structure(scratch), refs[len(names) :])
        for name, ref in [*zip(names, refs), *work.items()]:
            setattr(m, name, ref)
        t, d = lax.axis_index("tensor"), lax.axis_index("dp")
        a, b = lax.div(t, I), lax.rem(t, I)
        y, core = lax.div(d, C), lax.rem(d, C)
        place = (a, b)
        lane = lax.broadcasted_iota(jnp.int32, (1, LANES), 1)

        held, normed, W, WO, acc = m.held, m.normed, m.W, m.WO, m.acc

        def to_lanes(column):
            eye = lax.broadcasted_iota(jnp.int32, (R, z.Rp), 0) == lax.broadcasted_iota(
                jnp.int32, (R, z.Rp), 1
            )
            return jnp.sum(jnp.where(eye, column, 0.0), axis=0, keepdims=True)

        def to_column(row):
            eye = lax.broadcasted_iota(jnp.int32, (R, z.Rp), 0) == lax.broadcasted_iota(
                jnp.int32, (R, z.Rp), 1
            )
            return jnp.sum(jnp.where(eye, row, 0.0), axis=1, keepdims=True)

        def stack_rows(rows):
            index = lax.broadcasted_iota(jnp.int32, (8, z.Rp), 0)
            out = jnp.zeros((8, z.Rp), f32)
            for i, row in enumerate(rows):
                out = jnp.where(index == i, row, out)
            return out

        def chunks(fn, total=R):
            @pl.loop(0, total // z.step)
            def _(i):
                fn(pl.ds(pl.multiple_of(i * z.step, 16), z.step))

        emitted = []

        def emit(ref, out):
            copy = pltpu.make_async_copy(ref, out, m.emit[0].at[len(emitted)])
            copy.start()
            emitted.append(copy)

        def exchange(refs, count=T, axis="tensor", rank=t):
            return Exchange(axis, rank, count, *refs)

        loads = [
            (m.pol_hidden, held.at[t, pl.ds(0, R)]),
            (m.ref_hidden, held.at[t, pl.ds(R, R)]),
            (m.w_query, W.at[d, :, pl.ds(0, QC)]),
            (m.w_key, W.at[d, :, pl.ds(QC, KC)]),
            (m.value_projection, W.at[d, :, pl.ds(QC + KC, KC)]),
            (m.a_query, m.a_in.at[pl.ds(0, z.rank)]),
            (m.a_value, m.a_in.at[pl.ds(z.rank, z.rank)]),
            (m.w_out, WO.at[d]),
            (m.query_factor_hbm, m.query_second_factor),
            (m.value_factor_hbm, m.value_second_factor),
            (m.pre_rows, m.gains.at[pl.ds(0, T)]),
            (m.post_rows, m.gains.at[pl.ds(T, T)]),
            (m.readout_hbm, m.readout),
            (m.cosine_hbm, m.cosine),
            (m.sine_hbm, m.sine),
        ]
        copies = [
            pltpu.make_async_copy(src, dst, m.load[0].at[i]) for i, (src, dst) in enumerate(loads)
        ]
        for copy in copies:
            copy.start()

        barrier = pltpu.get_barrier_semaphore()
        for k in range(1, T):
            pl.semaphore_signal(
                barrier, inc=1, device_id={"tensor": lax.rem(t + k, T)}, device_id_type=MESH
            )
        for k in range(1, D):
            pl.semaphore_signal(
                barrier, inc=1, device_id={"dp": lax.rem(d + k, D)}, device_id_type=MESH
            )

        acc[...] = jnp.zeros_like(acc)
        for s in range(S):
            slot = lax.broadcasted_iota(jnp.int32, (L, 1), 0)
            m.liv[s * L : (s + 1) * L, :] = (slot < m.lengths[s]).astype(f32)

        def square(rows):
            x = held[t, rows, :].astype(f32)
            m.col[rows, :] = jnp.sum(x * x, axis=1, keepdims=True)

        stats0 = exchange(m.s0)
        copies[0].wait()
        copies[1].wait()
        chunks(square, 2 * R)
        stats0.own[...] = stack_rows([to_lanes(m.col[0:R]), to_lanes(m.col[R:])])
        stats0.box[t] = stats0.own[...]

        copies[5].wait()
        copies[6].wait()
        same = lax.broadcasted_iota(jnp.int32, (z.AR, z.AR), 0) == lax.broadcasted_iota(
            jnp.int32, (z.AR, z.AR), 1
        )
        W[d, :, NC:NW] = dot(m.a_in[...], same.astype(bf16), TN).astype(bf16)
        pl.semaphore_wait(barrier, T - 1 + D - 1)
        stats0.start()

        hid = [Gather(z, place, held, m.hid[model], model * R) for model in range(2)]
        hid[0].start()
        hid[1].start()

        def weight_copy(job, slot, piece, k, far):
            buf, (recv, across, beside) = job
            block = buf.at[slot, pl.ds(piece * PW, PW)]
            if far:
                send = across.at[(k - 1) * z.r + piece]
                rank = lax.rem(y + k, Y) * C + core
            else:
                send = beside.at[(lax.div(slot, C) * (C - 1) + k - 1) * z.r + piece]
                rank = y * C + lax.rem(core + k, C)
            return remote(block, block, send, recv.at[slot * z.r + piece], "dp", rank)

        def order_of(q):
            return lax.rem(b + 1 + q, z.r)

        def weights_start(job):
            for q in range(z.r):
                for k in range(1, Y):
                    weight_copy(job, d, order_of(q), k, True).start()
                for k in range(1, C):
                    weight_copy(job, d, order_of(q), k, False).start()

        def weights_wait(job, slot, piece):
            weight_copy(job, slot, piece, 1, Y > 1).wait_recv()

        def weights_relay(job, q):
            for jj in range(1, Y):
                slot = lax.rem(y + jj, Y) * C + core
                weights_wait(job, slot, order_of(q))
                for k in range(1, C):
                    weight_copy(job, slot, order_of(q), k, False).start()

        def weights_wait_core(job, yy, q):
            for k in range(1, C):
                weights_wait(job, yy * C + lax.rem(core + k, C), order_of(q))

        def weights_drain(job):
            for q in range(z.r):
                for k in range(1, Y):
                    weight_copy(job, d, order_of(q), k, True).wait_send()
                for yy in range(Y):
                    for k in range(1, C):
                        weight_copy(job, yy * C + core, order_of(q), k, False).wait_send()

        wq, wo = (W, m.wq), (WO, m.wo)
        for copy in copies[2:5]:
            copy.wait()
        weights_start(wq)
        copies[7].wait()
        weights_start(wo)
        for copy in copies[8:]:
            copy.wait()
        m.F[...] = jnp.zeros_like(m.F)
        m.F[0 : z.rank, 0:QC] = m.query_second_factor[...]
        m.F[z.rank :, QC:] = m.value_second_factor[...]

        stats0.wait()

        scale = lax.rsqrt(stats0.total() / z.W + NORM_EPS)
        m.scol[0:R, :] = to_column(scale[0:1])
        m.scol[R:, :] = to_column(scale[1:2])

        def normalise(model, slot):
            gain = m.gains[pl.ds(slot, 1), :]

            def one(rows):
                at = pl.ds(pl.multiple_of(model * R + rows.start, 16), rows.size)
                x = held[slot, at, :].astype(f32)
                normed[slot, at, :] = (x * m.scol[at, :] * gain).astype(bf16)

            chunks(one)

        def arrive(model, aa):
            hid[model].wait_inner(aa)

            @pl.loop(0, I)
            def _(bb):
                normalise(model, aa * I + bb)

        def project(model, slot):
            row, count = model * R, R
            ws, off = lax.div(slot, z.r), lax.rem(slot, z.r) * PW

            @pl.loop(0, NW // n_tile)
            def _(i):
                cols = pl.ds(pl.multiple_of(i * n_tile, LANES), n_tile)
                acc[row : row + count, cols] += dot(
                    normed[slot, row : row + count, :],
                    W[ws, pl.ds(pl.multiple_of(off, 16), PW), cols],
                )

        def project_group(model, aa, stages):
            @pl.loop(0, I)
            def _(bb):
                slot = aa * I + bb
                near = lax.div(lax.div(slot, z.r), C) == y
                first = lax.rem(slot, z.r) != order_of(z.r - 1)
                kinds = [
                    near,
                    jnp.logical_not(near) & first,
                    jnp.logical_not(near) & jnp.logical_not(first),
                ]
                wanted = kinds[stages[0]]
                for stage in stages[1:]:
                    wanted = wanted | kinds[stage]

                @pl.when(wanted)
                def _():
                    project(model, slot)

        side = jnp.minimum(a, O - 1 - a)

        def visit(j):
            turn = jnp.where(a <= O - 1 - a, 1, -1)
            inside = jnp.where(
                lax.rem(j, 2) == 1, a + turn * lax.div(j + 1, 2), a - turn * lax.div(j, 2)
            )
            outside = jnp.where(a <= O - 1 - a, a + j - side, a - j + side)
            return jnp.where(j <= 2 * side, inside, outside)

        for q in range(z.r):
            weights_wait_core(wq, y, q)

        @pl.loop(1, O)
        def _(j):
            hid[0].relay(visit(j))
            arrive(0, visit(j - 1))
            project_group(0, visit(j - 1), [0])

        for q in range(z.r - 1):
            weights_relay(wq, q)
            for jj in range(1, Y):
                weights_wait_core(wq, lax.rem(y + jj, Y), q)

        hid[1].relay(visit(1))
        arrive(0, visit(O - 1))
        project_group(0, visit(O - 1), [0])

        @pl.loop(0, O)
        def _(j):
            project_group(0, j, [1])

        @pl.loop(2, O)
        def _(j):
            hid[1].relay(visit(j))

        @pl.when(side > 0)
        def _():
            arrive(1, visit(0))
            project_group(1, visit(0), [0, 1])

        weights_relay(wq, z.r - 1)
        for jj in range(1, Y):
            weights_wait_core(wq, lax.rem(y + jj, Y), z.r - 1)

        @pl.loop(0, O)
        def _(j):
            project_group(0, j, [2])

        row_slot = lax.broadcasted_iota(jnp.int32, (L, L), 0)
        key_slot = lax.broadcasted_iota(jnp.int32, (L, L), 1)
        causal = key_slot <= row_slot

        def attend(model):
            base = model * R
            if model == 0:
                m.low[...] = acc[0:R, NC:NW].astype(bf16)
                m.added[...] = ADAPTER_SCALE * dot(m.low[...], m.F[...])

            @pl.loop(0, S)
            def _(s):
                rows = pl.ds(pl.multiple_of(base + s * L, 16), L)
                local = pl.ds(pl.multiple_of(s * L, 16), L)
                allowed = causal & (key_slot < m.lengths[s])
                allowed = jnp.concatenate([allowed.astype(f32)] * z.G, axis=0) > 0.5
                cosine, sine = m.cosine[...], m.sine[...]
                for k in range(z.KV):
                    head = slice(k * HEAD_SIZE, (k + 1) * HEAD_SIZE)
                    kh = acc[rows, QC + k * HEAD_SIZE : QC + (k + 1) * HEAD_SIZE]
                    vh = acc[rows, QC + KC + k * HEAD_SIZE : QC + KC + (k + 1) * HEAD_SIZE]
                    if model == 0:
                        vh = vh + m.added[local, QC + k * HEAD_SIZE : QC + (k + 1) * HEAD_SIZE]
                    kh = rope(kh, cosine, sine).astype(bf16)
                    vh = vh.astype(bf16)
                    queries = []
                    for g in range(z.G):
                        h = k * z.G + g
                        qh = acc[rows, h * HEAD_SIZE : (h + 1) * HEAD_SIZE]
                        if model == 0:
                            qh = qh + m.added[local, h * HEAD_SIZE : (h + 1) * HEAD_SIZE]
                        queries.append(rope(qh, cosine, sine).astype(bf16))
                    q2 = jnp.concatenate(queries, axis=0)
                    scores = dot(q2, kh, NT) * query_scale()
                    capped = SOFT_CAP * jnp.tanh(scores / SOFT_CAP)
                    weights = jnp.where(allowed, jnp.exp(capped), 0.0)
                    probs = weights / jnp.sum(weights, axis=1, keepdims=True)
                    out = dot(probs.astype(bf16), vh).astype(bf16)
                    for g in range(z.G):
                        h = k * z.G + g
                        m.mixed[rows, h * HEAD_SIZE : (h + 1) * HEAD_SIZE] = out[
                            g * L : (g + 1) * L
                        ]
                    if model == 0:
                        m.q2[s, k] = q2
                        m.kk[s, k] = kh
                        m.vv[s, k] = vh
                        m.probs[s, k] = probs
                        m.capped[s, k] = capped

        attend(0)

        def out_term(model):
            def term(slot):
                ws, off = lax.div(slot, z.r), lax.rem(slot, z.r) * PW
                return dot(
                    m.mixed[model * R : (model + 1) * R, :],
                    WO[ws, pl.ds(pl.multiple_of(off, 16), PW), :],
                    NT,
                )

            return term

        def reduce_of(bufs, sems, out, row):
            return Reduce(
                z,
                place,
                bufs,
                sems,
                m.piece,
                out,
                row,
            )

        red_pol = reduce_of(m.pol, m.pol_sems, m.summed, 0)
        red_ref = reduce_of(m.ref, m.ref_sems, m.summed, R)
        red_grad = reduce_of(m.pol, m.grad_sems, m.gnorm, 0)

        def near_first(j):
            yy, jj = lax.rem(y + lax.div(j, z.gp), Y), lax.rem(j, z.gp)
            low = yy * z.gp + jj
            high = yy * z.gp + z.gp - 1 - jj
            return jnp.where(2 * yy < Y, low, high)

        def far_first(j):
            return visit(O - 1 - j)

        def produce_range(red, first, last, order, term, ks):
            @pl.loop(first, last)
            def _(j):
                for k in ks:
                    red.produce(order(j), k, term)

        def collect_stage(red, j, order, distance=None):
            aa = order(j)
            ahead = jnp.where(aa > a, a, O - 1 - a)
            wanted = aa != a if distance is None else (aa != a) & (ahead == distance)

            @pl.when(wanted)
            def _():
                red.collect(aa)

        def collect_range(red, first, last, order, distance=None):
            @pl.loop(first, last)
            def _(j):
                collect_stage(red, j, order, distance)

        xs, own = list(range(1, I)), [0]
        for q in range(z.r):
            weights_wait_core(wo, y, q)
        produce_range(red_pol, 0, z.gp, near_first, out_term(0), xs + own)
        early = z.r if I != z.r else z.r - 1
        for q in range(early):
            weights_relay(wo, q)
            for jj in range(1, Y):
                weights_wait_core(wo, lax.rem(y + jj, Y), q)
        produce_range(red_pol, z.gp, O, near_first, out_term(0), xs)

        @pl.loop(0, O - 1)
        def _(j):
            @pl.when((j > 0) | (side == 0))
            def _():
                arrive(1, visit(j))
                project_group(1, visit(j), [0, 1])

            @pl.when(j == 1)
            def _():
                collect_range(red_pol, 0, 1, near_first, 0)

        collect_range(red_pol, 1, z.gp, near_first, 0)
        for q in range(early, z.r):
            weights_relay(wo, q)

        for q in range(early, z.r):
            for jj in range(1, Y):
                weights_wait_core(wo, lax.rem(y + jj, Y), q)
        produce_range(red_pol, z.gp, O, near_first, out_term(0), own)
        collect_range(red_pol, z.gp, z.gp + 1, near_first, 0)
        collect_range(red_pol, 0, z.gp, near_first, 1)
        arrive(1, visit(O - 1))
        project_group(1, visit(O - 1), [0, 1])

        @pl.loop(0, O)
        def _(j):
            project_group(1, j, [2])

        attend(1)
        produce_range(red_ref, 0, 2, far_first, out_term(1), xs + own)

        for distance in range(2, O - 1):
            collect_range(red_pol, 0, z.gp, near_first, distance)

        @pl.loop(1, O - 1 + 2 * (O - 1 - z.gp))
        def _(turn):
            @pl.loop(z.gp, O)
            def _(j):
                collect_stage(red_pol, j, near_first, turn - 2 * (j - z.gp))

        red_pol.collect(a)

        post_gain = m.gains[pl.ds(T + t, 1), :]

        def token_sums(model, refs):
            base = model * R

            def one(rows):
                at = pl.ds(base + rows.start, rows.size)
                x = m.summed[at, :]
                read = m.readout[rows, :].astype(f32)
                m.pcol[pl.ds(rows.start, rows.size), :] = jnp.sum(x * x, axis=1, keepdims=True)
                m.pcol[pl.ds(R + rows.start, rows.size), :] = jnp.sum(
                    x * (post_gain * read), axis=1, keepdims=True
                )
                h = held[t, at, :].astype(f32)
                m.pcol[pl.ds(2 * R + rows.start, rows.size), :] = jnp.sum(
                    h * read, axis=1, keepdims=True
                )

            chunks(one)
            done = exchange(refs)
            done.own[...] = stack_rows([to_lanes(m.pcol[i * R : (i + 1) * R]) for i in range(3)])
            done.box[t] = done.own[...]
            done.start()
            return done

        stats1 = token_sums(0, m.s1)
        produce_range(red_ref, 2, O - 1, far_first, out_term(1), xs + own)
        collect_range(red_ref, 0, 2, far_first, 0)
        stats1.wait()
        sums1 = stats1.total()
        post1 = lax.rsqrt(sums1[0:1] / z.W + NORM_EPS)
        m.col[0:R, :] = to_column(post1)
        m.col[R:, :] = to_column(post1 * post1 * post1 * sums1[1:2] / z.W)

        def make_grad(rows):
            read = m.readout[rows, :].astype(f32)
            value = m.col[rows, :] * post_gain * read - m.summed[rows, :] * m.col[
                pl.ds(R + rows.start, rows.size), :
            ]
            m.gheld[t, rows, :] = (value * m.liv[rows, :]).astype(bf16)

        chunks(make_grad)
        gag = Gather(z, place, m.gheld, m.gag)
        gag.start()

        def finish(model, out):
            def one(rows):
                at = pl.ds(model * R + rows.start, rows.size)
                h = held[t, at, :].astype(f32)
                out[rows, :] = (h + m.summed[at, :] * m.pcol[rows, :] * post_gain).astype(
                    bf16
                )

            chunks(one)

        m.pcol[0:R, :] = m.col[0:R, :]
        finish(0, m.policy_out)
        emit(m.policy_out, m.out_policy)
        m.gm[...] = jnp.zeros_like(m.gm)

        def back_out(aa):
            @pl.loop(0, I)
            def _(bb):
                slot = aa * I + bb
                ws, off = lax.div(slot, z.r), lax.rem(slot, z.r) * PW
                m.gm[...] += dot(
                    m.gheld[slot], WO[ws, pl.ds(pl.multiple_of(off, 16), PW), :]
                )

        collect_range(red_ref, 2, O - 1, far_first, 0)

        @pl.loop(1, O)
        def _(j):
            gag.relay(visit(j))

            @pl.when(j == O - 1)
            def _():
                produce_range(red_ref, O - 1, O, far_first, out_term(1), xs + own)

            gag.wait_inner(visit(j - 1))
            back_out(visit(j - 1))

        collect_range(red_ref, 0, O - 1, far_first, 1)
        gag.wait_inner(visit(O - 1))
        back_out(visit(O - 1))
        for distance in range(2, O - 1):
            collect_range(red_ref, 0, O - 1, far_first, distance)
        m.gmb[...] = m.gm[...].astype(bf16)

        @pl.loop(0, S)
        def _(s):
            rows = pl.ds(pl.multiple_of(s * L, 16), L)
            cosine, sine = m.cosine[...], -m.sine[...]
            for k in range(z.KV):
                parts = []
                for g in range(z.G):
                    h = k * z.G + g
                    parts.append(m.gmb[rows, h * HEAD_SIZE : (h + 1) * HEAD_SIZE])
                grad = jnp.concatenate(parts, axis=0)
                probs, capped = m.probs[s, k], m.capped[s, k]
                grad_probs = dot(grad, m.vv[s, k], NT)
                grad_v = dot(probs.astype(bf16), grad, TN)
                centered = grad_probs - jnp.sum(grad_probs * probs, axis=1, keepdims=True)
                ratio = capped / SOFT_CAP
                grad_scores = (
                    probs * centered * (1.0 - ratio * ratio) * query_scale()
                ).astype(bf16)
                grad_q = dot(grad_scores, m.kk[s, k])
                grad_k = dot(grad_scores, m.q2[s, k], TN)
                for g in range(z.G):
                    h = k * z.G + g
                    m.dcat[rows, h * HEAD_SIZE : (h + 1) * HEAD_SIZE] = rope(
                        grad_q[g * L : (g + 1) * L], cosine, sine
                    ).astype(bf16)
                at = QC + k * HEAD_SIZE
                m.dcat[rows, at : at + HEAD_SIZE] = rope(grad_k, cosine, sine).astype(bf16)
                m.dcat[rows, at + KC : at + KC + HEAD_SIZE] = grad_v.astype(bf16)

        m.dcat[:, NC:NW] = (
            ADAPTER_SCALE
            * (
                dot(m.dcat[:, 0:QC], m.F[:, 0:QC], NT)
                + dot(m.dcat[:, QC + KC : NC], m.F[:, QC:], NT)
            )
        ).astype(bf16)

        def in_term(slot):
            ws, off = lax.div(slot, z.r), lax.rem(slot, z.r) * PW
            return dot(m.dcat[...], W[ws, pl.ds(pl.multiple_of(off, 16), PW), :], NT)

        def pre_dot(rows):
            m.pcol[pl.ds(3 * R + rows.start, rows.size), :] = jnp.sum(
                m.dcat[rows, :].astype(f32) * acc[rows, :], axis=1, keepdims=True
            )

        def hook_part(part, k):
            return remote(
                m.dcat.at[pl.ds(pl.multiple_of(part * z.HR, 16), z.HR), pl.ds(NC, z.AR)],
                m.hbox.at[t],
                m.h1[0].at[k],
                m.h1[1].at[t],
                "tensor",
                lax.rem(t + k, T),
            )

        def hook_whole(k):
            mine = m.hsum.at[t]
            peer = lax.rem(t + k, T)
            return remote(mine, mine, m.h2[0].at[k], m.h2[1].at[t], "tensor", peer)

        for k in range(1, T):
            peer = lax.rem(t + k, T)

            @pl.when(peer < z.HN)
            def _(peer=peer, k=k):
                hook_part(peer, k).start()

        chunks(pre_dot)
        stats3 = exchange(m.s3)
        stats3.own[...] = stack_rows([to_lanes(m.pcol[3 * R :])])
        stats3.box[t] = stats3.own[...]
        stats3.start()
        red_pol.drain()
        produce_range(red_grad, 0, 1, far_first, in_term, xs + own)
        red_ref.collect(a)
        stats2 = token_sums(1, m.s2)
        produce_range(red_grad, 1, 2, far_first, in_term, xs + own)

        @pl.when(t < z.HN)
        def _():
            at = pl.ds(pl.multiple_of(t * z.HR, 16), z.HR)
            m.hbox[t] = m.dcat[at, NC:NW]
            for k in range(1, T):
                peer = lax.rem(t + k, T)
                slot = m.hbox.at[peer]
                remote(slot, slot, m.h1[0].at[k], m.h1[1].at[peer], "tensor", peer).wait_recv()
            value = m.hbox[0].astype(f32)
            for k in range(1, T):
                value += m.hbox[k].astype(f32)
            m.hsum[t] = value.astype(bf16)
            for k in range(1, T):
                hook_whole(k).start()

        produce_range(red_grad, 2, O - 1, far_first, in_term, xs + own)
        collect_range(red_grad, 0, 1, far_first)
        produce_range(red_grad, O - 1, O, far_first, in_term, xs + own)
        stats2.wait()
        sums2 = stats2.total()
        post2 = lax.rsqrt(sums2[0:1] / z.W + NORM_EPS)

        token_pol = sums1[2:3] + post1 * sums1[1:2]
        token_ref = sums2[2:3] + post2 * sums2[1:2]
        wide = lax.broadcasted_iota(jnp.int32, (1, z.Rp), 1)
        mine = jnp.zeros((1, LANES), f32)
        for s in range(S):
            inside = (wide >= s * L) & (wide < s * L + m.lengths[s])
            value = jnp.sum(jnp.where(inside, token_pol, 0.0), axis=1, keepdims=True) - jnp.sum(
                jnp.where(inside, token_ref, 0.0), axis=1, keepdims=True
            )
            mine = jnp.where(lane == d * S + s, value, mine)
        scores = exchange(m.score, D, "dp", d)
        scores.own[...] = jnp.broadcast_to(mine, (8, LANES))
        scores.box[d] = scores.own[...]
        scores.start()
        scores.wait()
        ratios = scores.total()[0:1]
        loss = jnp.zeros((1, 1), f32)
        coefficients = jnp.zeros((1, LANES), f32)
        for k in range(S * D // 2):
            chosen, rejected = m.pairing[2 * k], m.pairing[2 * k + 1]
            margin = DPO_BETA * (
                jnp.sum(jnp.where(lane == chosen, ratios, 0.0), axis=1, keepdims=True)
                - jnp.sum(jnp.where(lane == rejected, ratios, 0.0), axis=1, keepdims=True)
            )
            soft = jnp.exp(-jnp.abs(margin))
            loss += jnp.maximum(-margin, 0.0) + jnp.log1p(soft)
            sigmoid = jnp.where(margin > 0, soft, 1.0) / (1.0 + soft)
            pull = DPO_BETA * LOSS_SCALE * sigmoid
            coefficients += jnp.where(lane == rejected, pull, 0.0) - jnp.where(
                lane == chosen, pull, 0.0
            )
        m.dpo_loss[...] = jnp.broadcast_to(loss, (8, LANES))
        emit(m.dpo_loss, m.out_loss)
        own_coef = []
        for s in range(S):
            value = jnp.sum(jnp.where(lane == d * S + s, coefficients, 0.0), axis=1, keepdims=True)
            own_coef.append(value)
            m.ccol[s * L : (s + 1) * L, :] = jnp.broadcast_to(value, (L, 1))

        parts_q = jnp.zeros((z.rank, QC), f32)
        parts_v = jnp.zeros((z.rank, KC), f32)
        for s in range(S):
            rows = slice(s * L, (s + 1) * L)
            low = m.low[rows, :]
            parts_q += own_coef[s] * dot(low, m.dcat[rows, 0:QC], TN)[0 : z.rank]
            parts_v += own_coef[s] * dot(low, m.dcat[rows, QC + KC : NC], TN)[z.rank :]
        factors = exchange(m.fac, D, "dp", d)
        factors.own[:, 0:QC] = (ADAPTER_SCALE * parts_q).astype(bf16)
        factors.own[:, QC:] = (ADAPTER_SCALE * parts_v).astype(bf16)
        factors.box[d] = factors.own[...]
        factors.start()

        for k in range(1, T):
            peer = lax.rem(t + k, T)

            @pl.when(peer < z.HN)
            def _(peer=peer, k=k):
                slot = m.hsum.at[peer]
                remote(slot, slot, m.h2[0].at[k], m.h2[1].at[peer], "tensor", peer).wait_recv()

        hook = m.hsum[...].reshape(R, z.AR)
        hook = (hook.astype(f32) * m.ccol[...]).astype(bf16)
        adapters = exchange(m.ad, D, "dp", d)

        @pl.loop(0, T)
        def _(slot):
            ws, off = lax.div(slot, z.r), lax.rem(slot, z.r) * PW
            adapters.own[ws, pl.ds(pl.multiple_of(off, 16), PW), :] = dot(
                normed[slot, 0:R, :], hook, TN
            ).astype(bf16)

        adapters.box[d] = adapters.own[d]
        adapters.start()
        collect_range(red_grad, 1, O - 1, far_first)
        m.pcol[0:R, :] = to_column(post2)
        finish(1, m.reference_out)
        emit(m.reference_out, m.out_reference)
        stats3.wait()
        m.pcol[0:R, :] = to_column(stats3.total()[0:1])
        factors.wait()
        value = factors.total()
        m.query_factor_gradient[...] = value[:, 0:QC]
        m.value_factor_gradient[...] = value[:, QC:]
        emit(m.query_factor_gradient, m.out_query)
        emit(m.value_factor_gradient, m.out_value)
        red_grad.collect(a)

        pre_gain = m.gains[pl.ds(t, 1), :]

        def grad_in(rows):
            read = m.readout[rows, :].astype(f32) * m.liv[rows, :]
            scale = m.scol[rows, :]
            h = held[t, rows, :].astype(f32)
            value = (
                read
                + scale * pre_gain * m.gnorm[rows, :]
                - h * (scale * scale * m.pcol[rows, :] / z.W)
            )
            m.grad_hidden[rows, :] = (value * m.ccol[rows, :]).astype(bf16)

        chunks(grad_in)
        emit(m.grad_hidden, m.out_hidden)
        adapters.wait()

        def sum_adapters(rows):
            value = adapters.box[0, rows, :].astype(f32)
            for k in range(1, D):
                value += adapters.box[k, rows, :].astype(f32)
            m.grad_a[rows, :] = value

        size = pick(z.r * PW, (96, 48, 32, 16))

        @pl.loop(0, z.r * PW // size)
        def _(i):
            sum_adapters(pl.ds(pl.multiple_of(i * size, 16), size))

        emit(m.grad_a, m.out_adapter)

        hid[0].drain()
        hid[1].drain()
        gag.drain()
        red_ref.drain()
        red_grad.drain()
        weights_drain(wq)
        weights_drain(wo)
        for done in (stats0, stats1, stats2, stats3, scores, factors, adapters):
            done.drain()
        for k in range(1, T):
            peer = lax.rem(t + k, T)

            @pl.when(peer < z.HN)
            def _(peer=peer, k=k):
                hook_part(peer, k).wait_send()

        @pl.when(t < z.HN)
        def _():
            for k in range(1, T):
                hook_whole(k).wait_send()

        for copy in emitted:
            copy.wait()

    return kernel


def hand_over(arrays):
    count = len(arrays)
    shapes = [array.shape if array.shape != (8, LANES) else (1, 1) for array in arrays]

    def kernel(*refs):
        ins, outs, held = refs[:count], refs[count : 2 * count], refs[2 * count : 3 * count]
        came, left = refs[3 * count :]
        arrivals = [
            pltpu.make_async_copy(src, dst, came.at[i])
            for i, (src, dst) in enumerate(zip(ins, held))
        ]
        for copy in arrivals:
            copy.start()
        exits = []
        for i, copy in enumerate(arrivals):
            copy.wait()
            if shapes[i] == (1, 1):
                outs[i][...] = held[i][0:1, 0:1]
            else:
                exits.append(pltpu.make_async_copy(held[i], outs[i], left.at[i]))
                exits[-1].start()
        for copy in exits:
            copy.wait()

    hbm = pl.BlockSpec(memory_space=pl.ANY)
    return pl.pallas_call(
        kernel,
        name="hand_over",
        out_shape=[jax.ShapeDtypeStruct(s, a.dtype) for s, a in zip(shapes, arrays)],
        in_specs=[hbm] * count,
        out_specs=[pl.BlockSpec(memory_space=pltpu.VMEM) if s == (1, 1) else hbm for s in shapes],
        scratch_shapes=[pltpu.VMEM(a.shape, a.dtype) for a in arrays]
        + [pltpu.SemaphoreType.DMA((count,)), pltpu.SemaphoreType.DMA((count,))],
    )(*arrays)


def body(
    ref_hidden,
    pol_hidden,
    readout,
    lengths,
    pairing,
    pre_gain,
    post_gain,
    w_query,
    w_key,
    value_projection,
    w_out,
    a_query,
    a_value,
    query_second_factor,
    value_second_factor,
):
    z = Sizes(
        pol_hidden.shape[0],
        pol_hidden.shape[1],
        lengths.shape[0],
        lax.axis_size("dp"),
        lax.axis_size("tensor"),
        w_query.shape[1],
        w_key.shape[1],
        query_second_factor.shape[0],
    )
    cosine, sine = rope_tables(z.L)
    smem = pl.BlockSpec(memory_space=pltpu.SMEM)
    hbm = pl.BlockSpec(memory_space=pl.ANY)
    inputs = dict(
        pol_hidden=pol_hidden,
        ref_hidden=ref_hidden,
        readout_hbm=readout,
        lengths=lengths,
        pairing=pairing,
        pre_rows=pre_gain.reshape(z.T, z.PW),
        post_rows=post_gain.reshape(z.T, z.PW),
        w_query=w_query,
        w_key=w_key,
        value_projection=value_projection,
        w_out=w_out,
        a_query=a_query.T,
        a_value=a_value.T,
        query_factor_hbm=query_second_factor,
        value_factor_hbm=value_second_factor,
        cosine_hbm=jnp.asarray(cosine),
        sine_hbm=jnp.asarray(sine),
    )
    outputs = dict(
        out_policy=((z.R, z.PW), bf16),
        out_reference=((z.R, z.PW), bf16),
        out_loss=((8, LANES), f32),
        out_hidden=((z.R, z.PW), bf16),
        out_adapter=((z.r * z.PW, z.AR), f32),
        out_query=((z.rank, z.QC), f32),
        out_value=((z.rank, z.KC), f32),
    )
    scratch = build_scratch(z)
    outs = pl.pallas_call(
        make_kernel(z, [*inputs, *outputs], scratch),
        name="preference_step",
        out_shape=[jax.ShapeDtypeStruct(*entry) for entry in outputs.values()],
        in_specs=[smem if array.ndim == 1 else hbm for array in inputs.values()],
        out_specs=[hbm] * len(outputs),
        scratch_shapes=jax.tree.leaves(scratch),
        compiler_params=pltpu.CompilerParams(
            collective_id=1, has_side_effects=True, vmem_limit_bytes=VMEM_GRANT
        ),
    )(*inputs.values())
    policy_out, reference_out, loss, grad_hidden, grad_a, grad_q, grad_v = hand_over(outs)
    return policy_out, reference_out, loss[0, 0], grad_hidden, grad_a, grad_q, grad_v


def solution(mesh):
    placed = (
        P("dp", "tensor"),
        P("dp", "tensor"),
        P("dp", "tensor"),
        P("dp"),
        P(),
        P(),
        P(),
        P("dp", "tensor"),
        P("dp", "tensor"),
        P("dp", "tensor"),
        P("dp", "tensor"),
        P("dp", None),
        P("dp", None),
        P(None, "tensor"),
        P(None, "tensor"),
    )
    return jax.shard_map(
        body,
        mesh=mesh,
        in_specs=placed,
        out_specs=(
            P("dp", "tensor"),
            P("dp", "tensor"),
            P(),
            P("dp", "tensor"),
            P("dp", None),
            P(None, "tensor"),
            P(None, "tensor"),
        ),
        check_vma=False,
    )
```
